32 devices in a mesh: seq: 8 (over z, y), head: 4 (over x, core).
Axes of the slice: x: 2, y: 2, z: 4, core: 2. Of those that a mesh axis runs over, the one named last changes fastest.
Arguments:
- queries: bfloat16 [4096, 8192], P(('seq', 'head')), may hold values from -8 to 8
- keys: bfloat16 [4096, 1024], P(('seq', 'head')), may hold values from -8 to 8
- values: bfloat16 [4096, 1024], P(('seq', 'head')), may hold values from -6 to 6
- selected: int32 [32, 8], P('seq'), may hold values from 0 to 31, as said below
- counts: int32 [32], P('seq'), may hold values from 1 to 8
- block_slot: int32 [32], P('seq'), may hold values from 0 to 31, as said below
Outputs:
- attended: bfloat16 [4096, 8192], P(('seq', 'head'))
The draws below stay inside these ranges and needn't reach their ends.
Inputs may be any that keep to these rules, and one draw needn't show every extreme that they name: A permutation of 0 to 31. Block b's rows of keys and values start at row 128 * block_slot[b]; its owner shard is block_slot[b] // 4. The 4 blocks of one sequence shard (blocks s * 4 onward) have distinct owner shards, and block_slot[b] % 4 == b % 4. `selected`: row q lists its live entries first: entry 0 is q itself, the other live entries are distinct blocks of earlier sequence shards; entries from counts[q] on are 0. Over the live entries of the 4 rows of one sequence shard, at most 2 distinct blocks have the same owner shard, and in every draw some shard reaches 2 from some owner.
All inputs are finite; a program needn't handle non-finite values.
Results may differ from the reference program's by a relative error of at most 0.0049.
Values may be sent and summed in bfloat16 or wider, within the bound.
A program may use at most 128 MiB of HBM per device.

```python
import math
import jax
import jax.numpy as jnp
from jax import lax

QUERY_HEADS = 64
KEY_VALUE_HEADS = 8
HEAD_SIZE = 128
BLOCK_ROWS = 128
SELECTION_COUNT = 8
BLK_SEQ = 4
NB = 32
TOKEN_COUNT = 4096
N_SEQ = 8


def selection_tables(key):
    base = jax.random.fold_in(key, 4049)
    keys_list = jax.random.split(base, 5)
    shard_perm = jax.random.permutation(keys_list[0], N_SEQ).astype(jnp.int32)
    offsets = jax.random.permutation(keys_list[1], N_SEQ)[:BLK_SEQ].astype(jnp.int32)
    blocks = jnp.arange(NB, dtype=jnp.int32)
    home_shard = blocks // BLK_SEQ
    within = blocks % BLK_SEQ
    owner_of = (shard_perm[home_shard] + offsets[within]) % N_SEQ
    slot_of = owner_of * BLK_SEQ + within
    by_slot = jnp.zeros((NB,), jnp.int32).at[slot_of].set(blocks)
    slot_grid = by_slot.reshape(N_SEQ, BLK_SEQ)
    grid_shard = slot_grid // BLK_SEQ
    rank_draw = jax.random.randint(keys_list[2], (N_SEQ, N_SEQ, BLK_SEQ), 0, 1 << 20) * BLK_SEQ + jnp.arange(BLK_SEQ, dtype=jnp.int32)
    requesters = jnp.arange(N_SEQ, dtype=jnp.int32)[:, None, None]
    masked = jnp.where(grid_shard[None] < requesters, rank_draw, -1)
    best_pick = jnp.argmax(masked, axis=2).astype(jnp.int32)
    extra_ok = jnp.max(masked, axis=2) >= 0
    spread_grid = jnp.broadcast_to(slot_grid[None], (N_SEQ, N_SEQ, BLK_SEQ))
    extra_block = jnp.take_along_axis(spread_grid, best_pick[:, :, None], axis=2)[:, :, 0]
    priority = jax.random.randint(keys_list[3], (NB, N_SEQ), 0, 1 << 20) * N_SEQ + jnp.arange(N_SEQ, dtype=jnp.int32)[None, :]
    first_owner = owner_of[home_shard * BLK_SEQ]
    forced = (within == BLK_SEQ - 1)[:, None] & (jnp.arange(N_SEQ, dtype=jnp.int32)[None, :] == first_owner[:, None])
    priority = jnp.where(forced, 1 << 30, priority)
    usable = extra_ok[home_shard]
    priority = jnp.where(usable, priority, -1)
    top_values, top_index = lax.top_k(priority, SELECTION_COUNT - 1)
    picked = jnp.take_along_axis(extra_block[home_shard], top_index, axis=1)
    pool_size = jnp.sum(usable.astype(jnp.int32), axis=1)
    want_count = jax.random.randint(keys_list[4], (NB,), SELECTION_COUNT // 2, SELECTION_COUNT)
    extra_count = jnp.minimum(want_count, pool_size).astype(jnp.int32)
    position = jnp.arange(SELECTION_COUNT - 1, dtype=jnp.int32)[None, :]
    picked = jnp.where(position < extra_count[:, None], picked, 0).astype(jnp.int32)
    chosen = jnp.concatenate([blocks[:, None], picked], axis=1).astype(jnp.int32)
    return (slot_of.astype(jnp.int32), chosen, (1 + extra_count).astype(jnp.int32))


def draw_selected(key, part):
    return selection_tables(key)[1]


def draw_counts(key, part):
    return selection_tables(key)[2]


def draw_block_slot(key, part):
    return selection_tables(key)[0]


def draw_queries(key, part):
    random_portion = jax.random.normal(jax.random.fold_in(key, 11), (TOKEN_COUNT, QUERY_HEADS, HEAD_SIZE), jnp.float32)
    sampled_blocks = random_portion
    return jnp.clip(sampled_blocks, -8.0, 8.0).reshape(TOKEN_COUNT, QUERY_HEADS * HEAD_SIZE).astype(jnp.bfloat16)


def draw_keys(key, part):
    random_portion = jax.random.normal(jax.random.fold_in(key, 21), (TOKEN_COUNT, KEY_VALUE_HEADS, HEAD_SIZE), jnp.float32)
    sampled_blocks = random_portion
    return jnp.clip(sampled_blocks, -8.0, 8.0).reshape(TOKEN_COUNT, KEY_VALUE_HEADS * HEAD_SIZE).astype(jnp.bfloat16)


def shard_levels(stream_key, dims, pieces, least, largest):
    def one(dim, shards_of):
        heights = jax.random.uniform(jax.random.fold_in(jax.random.fold_in(stream_key, 6), dim), (shards_of,), jnp.float32, least / len(pieces), largest / len(pieces))
        return jnp.repeat(jnp.exp(heights), dims[dim] // shards_of).reshape((-1,) + (1,) * (len(dims) - dim - 1))

    level = one(*pieces[0])
    for cut in pieces[1:]:
        level = level * one(*cut)
    return level


def centred(key, dims, width, limit, cuts=(), kind=jnp.bfloat16):
    gain = shard_levels(key, dims, cuts, -0.22, 0.18) if cuts else 1.0
    entries = jax.random.normal(key, dims, jnp.float32) * width * gain
    return jnp.minimum(jnp.maximum(entries, -limit), limit).astype(kind)


def setup_inputs(seed: int = 0) -> dict:
    splits = jax.random.split(jax.random.key(seed), 7)
    queries = draw_queries(jax.random.fold_in(splits[6], 71), 0)
    keys = draw_keys(jax.random.fold_in(splits[6], 71), 0)
    values = centred(splits[2], (TOKEN_COUNT, KEY_VALUE_HEADS * HEAD_SIZE), 1.0, 6.0, ((0, 32),))
    selected = draw_selected(jax.random.fold_in(splits[6], 71), 0)
    counts = draw_counts(jax.random.fold_in(splits[6], 71), 0)
    block_slot = draw_block_slot(jax.random.fold_in(splits[6], 71), 0)
    return dict(queries=queries, keys=keys, values=values, selected=selected, counts=counts, block_slot=block_slot)


def reference(queries, keys, values, selected, counts, block_slot):
    block_count = selected.shape[0]
    heads_per_group = QUERY_HEADS // KEY_VALUE_HEADS
    score_scale = 1.0 / math.sqrt(HEAD_SIZE)
    key_block_list = keys.reshape(block_count, BLOCK_ROWS, KEY_VALUE_HEADS, HEAD_SIZE)
    value_block_list = values.reshape(block_count, BLOCK_ROWS, KEY_VALUE_HEADS, HEAD_SIZE)
    query_block_list = queries.reshape(block_count, BLOCK_ROWS, KEY_VALUE_HEADS, heads_per_group, HEAD_SIZE)

    def one_block(operands):
        block_id, query_tile, chosen, live_count = operands
        holder_shard = block_slot[chosen]
        key_block_rows = key_block_list[holder_shard].reshape(SELECTION_COUNT * BLOCK_ROWS, KEY_VALUE_HEADS, HEAD_SIZE)
        value_block_rows = value_block_list[holder_shard].reshape(SELECTION_COUNT * BLOCK_ROWS, KEY_VALUE_HEADS, HEAD_SIZE)
        scores = jnp.einsum('igmd,kgd->gmik', query_tile.astype(jnp.float32), key_block_rows.astype(jnp.float32)) * score_scale
        query_pos = block_id * BLOCK_ROWS + jnp.arange(BLOCK_ROWS, dtype=jnp.int32)
        key_pos = (chosen[:, None] * BLOCK_ROWS + jnp.arange(BLOCK_ROWS, dtype=jnp.int32)[None, :]).reshape(-1)
        live_entry = jnp.repeat(jnp.arange(SELECTION_COUNT, dtype=jnp.int32) < live_count, BLOCK_ROWS)
        visible = live_entry[None, :] & (key_pos[None, :] <= query_pos[:, None])
        scores = jnp.where(visible[None, None], scores, -jnp.inf)
        row_top = lax.optimization_barrier(jnp.max(scores, axis=-1, keepdims=True))
        weights = jnp.exp(scores - row_top)
        probability = (weights / lax.optimization_barrier(jnp.sum(weights, axis=-1, keepdims=True))).astype(jnp.bfloat16)
        mixed_out = jnp.einsum('gmik,kgd->igmd', probability.astype(jnp.float32), value_block_rows.astype(jnp.float32))
        return mixed_out.astype(jnp.bfloat16).reshape(BLOCK_ROWS, QUERY_HEADS * HEAD_SIZE)
    attended = lax.map(one_block, (jnp.arange(block_count, dtype=jnp.int32), query_block_list, selected, counts))
    return attended.reshape(block_count * BLOCK_ROWS, QUERY_HEADS * HEAD_SIZE)
```

```python
import functools
import math

import jax
import jax.numpy as jnp
from jax import lax
from jax.experimental import pallas as pl
from jax.experimental.pallas import tpu as pltpu
from jax.sharding import PartitionSpec as P

QUERY_HEADS = 64
KEY_VALUE_HEADS = 8
HEAD_SIZE = 128
BLOCK_ROWS = 128
Y_SIZE = 2
PER_OWNER = 2
MESH = pl.DeviceIdType.MESH


def kernel(ns, nh, groups, entries, q_ref, k_ref, v_ref, sel_ref, cnt_ref, own_slot_ref, out_ref,
           qbuf, obuf, kcat, vcat, diag, stage, row_ref, rows_v, rows_s, plan_v, plan_s,
           hs, hr, qs, qr, us, ur, ds_, dr, ys, yr, os_, or_, ss, sr, local_sem, *kv):
    s = lax.axis_index("seq")
    h = lax.axis_index("head")
    ysz = Y_SIZE
    zsz = ns // ysz
    z = s // ysz
    y = s % ysz
    y_peer = s + 1 - 2 * y
    half = nh // 2
    side = h // half
    spot = h % half
    width = qbuf.shape[3]
    heads_per_group = width // HEAD_SIZE
    blk_seq = sel_ref.shape[0]
    near = [(0, i) for i in range(1, half)]
    far = [(1, i) for i in range(half)]
    ways = near + far

    def remote(src, dst, send, recv, dev):
        return pltpu.make_async_remote_copy(
            src_ref=src, dst_ref=dst, send_sem=send, recv_sem=recv,
            device_id=dev, device_id_type=MESH)

    def target(w):
        flip, i = ways[w]
        return (side + flip) % 2 * half + (spot + i) % half

    def origin(w):
        flip, i = ways[w]
        return (side + flip) % 2 * half + (spot + half - i) % half

    lane = lax.broadcasted_iota(jnp.int32, (1, 128), 1)
    info = jnp.zeros((1, 128), jnp.int32)
    for j in range(blk_seq):
        info = jnp.where(lane == j, own_slot_ref[j], info)
        for e in range(entries):
            block = jnp.where(e < cnt_ref[j], sel_ref[j, e], sel_ref[j, 0])
            info = jnp.where(lane == blk_seq + j * entries + e, block, info)
    row_ref[...] = info

    barrier = pltpu.get_barrier_semaphore()
    for d in range(1, nh):
        pl.semaphore_signal(barrier, inc=1, device_id=(s, (h + d) % nh), device_id_type=MESH)
    for d in range(1, ns):
        pl.semaphore_signal(barrier, inc=1, device_id=((s + d) % ns, h), device_id_type=MESH)
    pl.semaphore_wait(barrier, nh - 1 + ns - 1)

    def lanes(unit, size):
        return pl.ds(pl.multiple_of(unit * size, size), size)

    def kv_head(g, t, w, peer, place):
        src = (k_ref, v_ref)[t]
        return remote(src.at[:, lanes(peer * groups + g, HEAD_SIZE)], kv[g].at[z * nh + place, t],
                      hs.at[g, t, w], hr.at[g, t, w], (s, peer))

    def kv_head_out(g, t, w):
        return kv_head(g, t, w, target(w), h)

    def kv_head_in(g, t, w):
        return kv_head(g, t, w, origin(w), origin(w))

    def q_head(g, w, peer, place):
        return remote(q_ref.at[:, lanes(peer * groups + g, width)], qbuf.at[g, place],
                      qs.at[g, w], qr.at[g, w], (s, peer))

    def q_head_out(g, w):
        return q_head(g, w, target(w), h)

    def q_head_in(g, w):
        return q_head(g, w, origin(w), origin(w))

    def row_out(d):
        return remote(row_ref, rows_v.at[s], ss.at[d - 1], sr.at[d - 1], ((s + d) % ns, h))

    def row_in(d):
        peer = (s + ns - d) % ns
        return remote(row_ref, rows_v.at[peer], ss.at[d - 1], sr.at[d - 1], (peer, h))

    for g in range(groups):
        for w in range(len(ways)):
            for t in range(2):
                kv_head_out(g, t, w).start()
        if g == 0:
            for d in range(1, ns):
                row_out(d).start()
    for g in range(groups):
        for w in reversed(range(len(ways))):
            q_head_out(g, w).start()

    for g in range(groups):
        kv[g][z * nh + h, 0] = k_ref[:, lanes(h * groups + g, HEAD_SIZE)]
        kv[g][z * nh + h, 1] = v_ref[:, lanes(h * groups + g, HEAD_SIZE)]
        qbuf[g, h] = q_ref[:, lanes(h * groups + g, width)]
    rows_v[s] = row_ref[...]
    pair_rows = 2 * BLOCK_ROWS
    row = lax.rem(lax.broadcasted_iota(jnp.int32, (pair_rows, BLOCK_ROWS), 0), BLOCK_ROWS)
    col = lax.broadcasted_iota(jnp.int32, (pair_rows, BLOCK_ROWS), 1)
    diag[...] = jnp.where(col <= row, 0.0, -jnp.inf).astype(jnp.float32)
    vcat[:, HEAD_SIZE:] = jnp.ones((entries * BLOCK_ROWS, HEAD_SIZE), jnp.bfloat16)

    def part(g, zz, p):
        lo = (side + p) % 2 * half
        return kv[g].at[pl.ds(zz * nh + lo, half)]

    def up(g, p, t, zz, dev):
        ref = part(g, zz, p)
        return remote(ref, ref, us.at[g, p, t], ur.at[g, p, t], (dev, h))

    def down(g, p, t, zz, dev):
        ref = part(g, zz, p)
        return remote(ref, ref, ds_.at[g, p, t], dr.at[g, p, t], (dev, h))

    def across(g, r, zz):
        return remote(stage.at[g, pl.ds(zz * PER_OWNER, PER_OWNER)],
                      kv[g].at[pl.ds(zsz * nh + zz * PER_OWNER, PER_OWNER)],
                      ys.at[g, r], yr.at[g, r], (y_peer, h))

    def send_across(g, r, zz):
        for k in range(PER_OWNER):
            pick = plan_s[1 + k, r]
            for t in range(2):
                chosen = kv[g][zz * nh + nh - 1, t]
                for j in reversed(range(nh - 1)):
                    chosen = jnp.where(pick == j, kv[g][zz * nh + j, t], chosen)
                stage[g, zz * PER_OWNER + k, t] = chosen
        across(g, r, zz).start()

    def send_both(g, p):
        if zsz > 1:
            @pl.when(z < zsz - 1)
            def _():
                up(g, p, 0, z, s + ysz).start()

            @pl.when(z > 0)
            def _():
                down(g, p, 0, z, s - ysz).start()

    def gather_z(g):
        for w in range(len(ways)):
            if w == len(near):
                send_both(g, 0)
            for t in range(2):
                kv_head_in(g, t, w).wait_recv()
        send_both(g, 1)

    def gather_step(g, t):
        @pl.when(z - 1 - t >= 0)
        def _():
            below = z - 1 - t
            for p in range(2):
                up(g, p, t, below, s).wait_recv()
                if t + 1 < zsz - 1:
                    @pl.when(z < zsz - 1)
                    def _():
                        up(g, p, t + 1, below, s + ysz).start()
            send_across(g, 1 + t, below)

        @pl.when(z + 1 + t <= zsz - 1)
        def _():
            above = z + 1 + t
            for p in range(2):
                down(g, p, t, above, s).wait_recv()
                if t + 1 < zsz - 1:
                    @pl.when(z > 0)
                    def _():
                        down(g, p, t + 1, above, s - ysz).start()
            send_across(g, zsz + t, above)

    def each_owner(call):
        call(0, z)
        for t in range(zsz - 1):
            @pl.when(z - 1 - t >= 0)
            def _():
                call(1 + t, z - 1 - t)

            @pl.when(z + 1 + t <= zsz - 1)
            def _():
                call(zsz + t, z + 1 + t)

    def gather_end(g):
        each_owner(lambda r, zz: across(g, r, zz).wait_recv())

    def gather_drain(g):
        each_owner(lambda r, zz: across(g, r, zz).wait_send())
        for p in range(2):
            for t in range(zsz - 1):
                @pl.when((z < zsz - 1) & (z - t >= 0))
                def _():
                    up(g, p, t, z - t, s + ysz).wait_send()

                @pl.when((z > 0) & (z + t <= zsz - 1))
                def _():
                    down(g, p, t, z + t, s - ysz).wait_send()

    def plan():
        for d in range(1, ns):
            row_in(d).wait_recv()
        table = pltpu.make_async_copy(rows_v, rows_s, local_sem)
        table.start()
        table.wait()

        def slot_of(shard, i):
            b = rows_s[shard, 0, blk_seq + i]
            slot = rows_s[lax.div(b, blk_seq), 0, lax.rem(b, blk_seq)]
            owner = lax.div(slot, nh)
            return lax.rem(slot, nh), lax.div(owner, ysz), lax.rem(owner, ysz)

        first = jnp.full((1, 128), nh, jnp.int32)
        last = jnp.full((1, 128), -1, jnp.int32)
        for i in range(blk_seq * entries):
            j, oz, oy = slot_of(y_peer, i)
            r = jnp.where(oz < z, z - oz, jnp.where(oz > z, zsz - 1 + oz - z, 0))
            hit = lane == jnp.where(oy == y, r, -1)
            first = jnp.where(hit, jnp.minimum(first, j), first)
            last = jnp.where(hit, jnp.maximum(last, j), last)
        mine = [slot_of(s, i) for i in range(blk_seq * entries)]
        js = jnp.zeros((1, 128), jnp.int32)
        ozs = jnp.zeros((1, 128), jnp.int32)
        oys = jnp.zeros((1, 128), jnp.int32)
        for i, (j, oz, oy) in enumerate(mine):
            js = jnp.where(lane == i, j, js)
            ozs = jnp.where(lane == i, oz, ozs)
            oys = jnp.where(lane == i, oy, oys)
        second = jnp.zeros((1, 128), jnp.int32)
        for j, oz, oy in mine:
            second = jnp.where((ozs == oz) & (oys == oy) & (js > j), 1, second)
        place = jnp.where(oys == y, ozs * nh + js, zsz * nh + ozs * PER_OWNER + second)
        plan_v[0:1, :] = place
        plan_v[1:2, :] = first
        plan_v[2:3, :] = last
        copy = pltpu.make_async_copy(plan_v, plan_s, local_sem)
        copy.start()
        copy.wait()

    factor = math.log2(math.e) / math.sqrt(HEAD_SIZE)

    def fetch(g, j):
        for e in range(entries):
            place = plan_s[0, j * entries + e]
            rows = slice(e * BLOCK_ROWS, (e + 1) * BLOCK_ROWS)
            kcat[rows, :] = kv[g][place, 0]
            vcat[rows, :HEAD_SIZE] = kv[g][place, 1]

    def attend(g, j):
        rest = lax.broadcasted_iota(jnp.int32, (1, (entries - 1) * BLOCK_ROWS), 1) + BLOCK_ROWS
        bias = jnp.where(rest < cnt_ref[j] * BLOCK_ROWS, 0.0, -jnp.inf).astype(jnp.float32)

        def pair(i, _):
            cols = pl.multiple_of(i * 2 * HEAD_SIZE, 2 * HEAD_SIZE)
            q2 = qbuf[g, j, :, pl.ds(cols, 2 * HEAD_SIZE)]
            q2 = jnp.concatenate([q2[:, :HEAD_SIZE], q2[:, HEAD_SIZE:]], axis=0)
            scores = lax.dot_general(q2, kcat[...], (((1,), (1,)), ((), ())),
                                     preferred_element_type=jnp.float32)
            own = scores[:, :BLOCK_ROWS] + diag[...]
            others = scores[:, BLOCK_ROWS:] + bias
            scores = jnp.concatenate([own, others], axis=1)
            top = jnp.max(scores, axis=1, keepdims=True)
            weights = jnp.exp2((scores - top) * factor).astype(jnp.bfloat16)
            mixed = jnp.dot(weights, vcat[...], preferred_element_type=jnp.float32)
            result = (mixed[:, :HEAD_SIZE] / mixed[:, HEAD_SIZE:]).astype(jnp.bfloat16)
            obuf[g, j, :, pl.ds(cols, HEAD_SIZE)] = result[:BLOCK_ROWS]
            obuf[g, j, :, pl.ds(cols + HEAD_SIZE, HEAD_SIZE)] = result[BLOCK_ROWS:]
            return 0

        lax.fori_loop(0, heads_per_group // 2, pair, 0, unroll=True)

    def result(g, w, peer, mine):
        return remote(obuf.at[g, peer], out_ref.at[:, lanes(mine * groups + g, width)],
                      os_.at[g, w], or_.at[g, w], (s, peer))

    def result_out(g, w):
        return result(g, w, target(w), h)

    def result_in(g, w):
        return result(g, w, origin(w), origin(w))

    def back(w):
        flip, i = ways[w]
        return ways.index((flip, (half - i) % half))

    order = list(range(len(near), len(ways))) + list(range(len(near))) + [None]
    gather_z(0)
    plan()
    send_across(0, 0, z)
    for t in range(zsz - 2):
        gather_step(0, t)
    pending = None
    for g in range(groups):
        more = g + 1 < groups
        if more:
            gather_z(g + 1)
        if g == 0 and zsz > 1:
            gather_step(0, zsz - 2)
        steps = []
        if more:
            send_across(g + 1, 0, z)
            steps = list(range(zsz - 1))
            if steps:
                gather_step(g + 1, steps.pop(0))
        gather_end(g)
        for n, w in enumerate(order):
            own = w is None
            j = h if own else target(w)
            fetch(g, j)
            if pending is not None:
                result_out(*pending).start()
                pending = None
            if not own:
                q_head_in(g, back(w)).wait_recv()
            if n >= len(order) // 2 and len(steps) > 1:
                gather_step(g + 1, steps.pop(0))
            attend(g, j)
            if own:
                out_ref[:, lanes(h * groups + g, width)] = obuf[g, h]
            else:
                pending = (g, w)
        for t in steps:
            gather_step(g + 1, t)

    for g in range(groups):
        gather_drain(g)
        for w in range(len(ways)):
            for t in range(2):
                kv_head_out(g, t, w).wait_send()
            q_head_out(g, w).wait_send()
    for d in range(1, ns):
        row_out(d).wait_send()
    for g in range(groups):
        for w in range(len(ways)):
            result_out(g, w).wait_send()
            result_in(g, w).wait_recv()


def body(queries, keys, values, selected, counts, block_slot):
    ns = lax.axis_size("seq")
    nh = lax.axis_size("head")
    blk_seq, entries = selected.shape
    rows = queries.shape[0]
    groups = keys.shape[1] // HEAD_SIZE // nh
    width = queries.shape[1] // nh // groups
    assert rows == BLOCK_ROWS and blk_seq == nh and nh % 2 == 0 and ns % Y_SIZE == 0
    vmem = pl.BlockSpec(memory_space=pltpu.VMEM)
    smem = pl.BlockSpec(memory_space=pltpu.SMEM)
    zsz = ns // Y_SIZE
    dma = pltpu.SemaphoreType.DMA
    steps = max(zsz - 1, 1)
    held = zsz * (nh + PER_OWNER)
    return pl.pallas_call(
        functools.partial(kernel, ns, nh, groups, entries),
        out_shape=jax.ShapeDtypeStruct(queries.shape, jnp.bfloat16),
        in_specs=[vmem, vmem, vmem, smem, smem, smem],
        out_specs=vmem,
        scratch_shapes=[
            pltpu.VMEM((groups, nh, rows, width), jnp.bfloat16),
            pltpu.VMEM((groups, nh, rows, width), jnp.bfloat16),
            pltpu.VMEM((entries * BLOCK_ROWS, HEAD_SIZE), jnp.bfloat16),
            pltpu.VMEM((entries * BLOCK_ROWS, 2 * HEAD_SIZE), jnp.bfloat16),
            pltpu.VMEM((2 * BLOCK_ROWS, BLOCK_ROWS), jnp.float32),
            pltpu.VMEM((groups, zsz * PER_OWNER, 2, BLOCK_ROWS, HEAD_SIZE), jnp.bfloat16),
            pltpu.VMEM((1, 128), jnp.int32),
            pltpu.VMEM((ns, 1, 128), jnp.int32),
            pltpu.SMEM((ns, 1, 128), jnp.int32),
            pltpu.VMEM((8, 128), jnp.int32),
            pltpu.SMEM((8, 128), jnp.int32),
            dma((groups, 2, nh - 1)), dma((groups, 2, nh - 1)),
            dma((groups, nh - 1)), dma((groups, nh - 1)),
            dma((groups, 2, steps)), dma((groups, 2, steps)),
            dma((groups, 2, steps)), dma((groups, 2, steps)),
            dma((groups, 2 * zsz)), dma((groups, 2 * zsz)),
            dma((groups, nh - 1)), dma((groups, nh - 1)),
            dma((ns - 1,)), dma((ns - 1,)),
            dma,
        ] + [pltpu.VMEM((held, 2, BLOCK_ROWS, HEAD_SIZE), jnp.bfloat16)] * groups,
        compiler_params=pltpu.CompilerParams(
            collective_id=0, has_side_effects=True, vmem_limit_bytes=60 * 1024 * 1024),
        name="block_attention",
    )(queries, keys, values, selected, counts, block_slot)


def solution(mesh):
    return jax.shard_map(
        body,
        mesh=mesh,
        in_specs=(
            P(("seq", "head"), None),
            P(("seq", "head"), None),
            P(("seq", "head"), None),
            P("seq", None),
            P("seq"),
            P("seq"),
        ),
        out_specs=P(("seq", "head"), None),
        check_vma=False,
    )
```

```python
import functools
import math

import jax
import jax.numpy as jnp
from jax import lax
from jax.experimental import pallas as pl
from jax.experimental.pallas import tpu as pltpu
from jax.sharding import PartitionSpec as P

QUERY_HEADS = 64
KEY_VALUE_HEADS = 8
HEAD_SIZE = 128
BLOCK_ROWS = 128
Y_SIZE = 2
PER_OWNER = 2
MESH = pl.DeviceIdType.MESH


def kernel(ns, nh, heads, entries, q_hbm, k_hbm, v_hbm, sel_ref, cnt_ref, own_slot_ref, out_ref,
           qv, kvin, qbuf, obuf, kcat, vcat, diag, stage, rows_v, rows_s, plan_v, plan_s, place_v, place_s,
           ins, local_sem, hs, hr, qs, qr, us, ur, ds_, dr, ys, yr, cs, cr, os_, or_, ss, sr, *kv):
    s = lax.axis_index("seq")
    h = lax.axis_index("head")
    ysz = Y_SIZE
    zsz = ns // ysz
    hops = max(zsz - 1, 1)
    z = s // ysz
    y = s % ysz
    y_peer = s + 1 - 2 * y
    half = nh // 2
    side = h // half
    c = h % half
    partner = side * half + 1 - c
    x_peer = (1 - side) * half + c
    width = qbuf.shape[2]
    pairs = width // (2 * HEAD_SIZE)
    blk_seq = sel_ref.shape[0]

    def remote(src, dst, send, recv, dev):
        return pltpu.make_async_remote_copy(
            src_ref=src, dst_ref=dst, send_sem=send, recv_sem=recv,
            device_id=dev, device_id_type=MESH)

    def lanes(unit, size):
        return pl.ds(pl.multiple_of(unit * size, size), size)

    loads = [pltpu.make_async_copy(k_hbm, kvin.at[0], ins.at[0]),
             pltpu.make_async_copy(v_hbm, kvin.at[1], ins.at[1]),
             pltpu.make_async_copy(q_hbm, qv, ins.at[2])]
    for load in loads:
        load.start()

    barrier = pltpu.get_barrier_semaphore()
    for d in range(1, nh):
        pl.semaphore_signal(barrier, inc=1, device_id=(s, (h + d) % nh), device_id_type=MESH)
    pl.semaphore_signal(barrier, inc=1, device_id=(y_peer, h), device_id_type=MESH)

    @pl.when(z < zsz - 1)
    def _():
        pl.semaphore_signal(barrier, inc=1, device_id=(s + ysz, h), device_id_type=MESH)

    @pl.when(z > 0)
    def _():
        pl.semaphore_signal(barrier, inc=1, device_id=(s - ysz, h), device_id_type=MESH)

    lane = lax.broadcasted_iota(jnp.int32, (1, 128), 1)
    info = jnp.zeros((1, 128), jnp.int32)
    for j in range(blk_seq):
        info = jnp.where(lane == j, own_slot_ref[j], info)
        for e in range(entries):
            block = jnp.where(e < cnt_ref[j], sel_ref[j, e], sel_ref[j, 0])
            info = jnp.where(lane == blk_seq + j * entries + e, block, info)
    rows_v[y, z] = info
    pair_rows = 2 * BLOCK_ROWS
    row = lax.rem(lax.broadcasted_iota(jnp.int32, (pair_rows, BLOCK_ROWS), 0), BLOCK_ROWS)
    col = lax.broadcasted_iota(jnp.int32, (pair_rows, BLOCK_ROWS), 1)
    diag[...] = jnp.where(col <= row, 0.0, -jnp.inf).astype(jnp.float32)
    vcat[:, HEAD_SIZE:] = jnp.ones((entries * BLOCK_ROWS, HEAD_SIZE), jnp.bfloat16)

    pl.semaphore_wait(barrier, nh + jnp.where(z < zsz - 1, 1, 0) + jnp.where(z > 0, 1, 0))

    def row_side(column):
        return remote(rows_v.at[column], rows_v.at[column], ss.at[0], sr.at[0], (y_peer, h))

    def row_up(t, zz, dev):
        ref = rows_v.at[y, zz]
        return remote(ref, ref, ss.at[1 + t], sr.at[1 + t], (dev, h))

    def row_down(t, zz, dev):
        ref = rows_v.at[y, zz]
        return remote(ref, ref, ss.at[1 + hops + t], sr.at[1 + hops + t], (dev, h))

    def head_near(g, role, place):
        return remote(kvin.at[role, :, lanes(side * heads + g, HEAD_SIZE)],
                      kv[g].at[role, z * nh + place],
                      hs.at[g, 0], hr.at[g, 0], (s, partner))

    def head_far(g, role):
        return remote(kvin.at[role, :, lanes((1 - side) * heads + g, HEAD_SIZE)],
                      kv[g].at[role, z * nh + h],
                      hs.at[g, 1 + role], hr.at[g, 1 + c], (s, (1 - side) * half + role))

    def head_far_in(g, spot):
        return remote(kvin.at[0, :, lanes(0, HEAD_SIZE)],
                      kv[g].at[c, z * nh + (1 - side) * half + spot],
                      hs.at[g, 1 + spot], hr.at[g, 1 + spot], (s, (1 - side) * half + spot))

    def q_head(g):
        return remote(qv.at[:, lanes((1 - side) * heads + g, width)], qbuf.at[g],
                      qs.at[g], qr.at[g], (s, x_peer))

    def part(g, zz, p):
        lo = (side + p) % 2 * half
        return kv[g].at[c, pl.ds(zz * nh + lo, half)]

    def up(g, p, t, zz, dev):
        ref = part(g, zz, p)
        return remote(ref, ref, us.at[g, p, t], ur.at[g, p, t], (dev, h))

    def down(g, p, t, zz, dev):
        ref = part(g, zz, p)
        return remote(ref, ref, ds_.at[g, p, t], dr.at[g, p, t], (dev, h))

    def across(g, r, zz):
        return remote(stage.at[g % 2, pl.ds(zz * PER_OWNER, PER_OWNER)],
                      kv[g].at[c, pl.ds(zsz * nh + zz * PER_OWNER, PER_OWNER)],
                      ys.at[g, r], yr.at[g, r], (y_peer, h))

    def share(g, r, zz, role):
        ref = kv[g].at[role, pl.ds(zz * nh, nh)]
        return remote(ref, ref, cs.at[g, 0, r], cr.at[g, 0, r], (s, partner))

    def share_far(g, r, zz, role):
        ref = kv[g].at[role, pl.ds(zsz * nh + zz * PER_OWNER, PER_OWNER)]
        return remote(ref, ref, cs.at[g, 1, r], cr.at[g, 1, r], (s, partner))

    def pass_on(g, r, zz):
        for k in range(PER_OWNER):
            pick = plan_s[k, r]
            chosen = kv[g][c, zz * nh + nh - 1]
            for j in reversed(range(nh - 1)):
                chosen = jnp.where(pick == j, kv[g][c, zz * nh + j], chosen)
            stage[g % 2, zz * PER_OWNER + k] = chosen
        across(g, r, zz).start()
        share(g, r, zz, c).start()

    def take_far(g, r, zz):
        across(g, r, zz).wait_recv()
        share_far(g, r, zz, c).start()

    def owners(t, call):
        @pl.when(z - 1 - t >= 0)
        def _():
            call(1 + t, z - 1 - t)

        @pl.when(z + 1 + t <= zsz - 1)
        def _():
            call(zsz + t, z + 1 + t)

    def every_owner(call):
        call(0, z)
        for t in range(zsz - 1):
            owners(t, call)

    def send_both(g, p):
        if zsz > 1:
            @pl.when(z < zsz - 1)
            def _():
                up(g, p, 0, z, s + ysz).start()

            @pl.when(z > 0)
            def _():
                down(g, p, 0, z, s - ysz).start()

    def open_near(g):
        head_near(g, c, partner).wait_recv()
        send_both(g, 0)

    def open_far(g):
        for spot in range(half):
            head_far_in(g, spot).wait_recv()
        send_both(g, 1)

    def open_z(g):
        open_near(g)
        open_far(g)

    def open_y(g):
        if g >= 2:
            every_owner(lambda r, zz: across(g - 2, r, zz).wait_send())
        pass_on(g, 0, z)

    def step(g, t):
        @pl.when(z - 1 - t >= 0)
        def _():
            below = z - 1 - t
            for p in range(2):
                up(g, p, t, below, s).wait_recv()
                if t + 1 < zsz - 1:
                    @pl.when(z < zsz - 1)
                    def _():
                        up(g, p, t + 1, below, s + ysz).start()

        @pl.when(z + 1 + t <= zsz - 1)
        def _():
            above = z + 1 + t
            for p in range(2):
                down(g, p, t, above, s).wait_recv()
                if t + 1 < zsz - 1:
                    @pl.when(z > 0)
                    def _():
                        down(g, p, t + 1, above, s - ysz).start()

    def side_step(g, t):
        owners(t, lambda r, zz: pass_on(g, r, zz))

    def take_step(g, t):
        if t < 0:
            take_far(g, 0, z)
        else:
            owners(t, lambda r, zz: take_far(g, r, zz))

    def close(g):
        every_owner(lambda r, zz: share(g, r, zz, 1 - c).wait_recv())
        every_owner(lambda r, zz: share_far(g, r, zz, 1 - c).wait_recv())

    def drain(g):
        head_near(g, 1 - c, h).wait_send()
        for role in range(2):
            head_far(g, role).wait_send()
        q_head(g).wait_send()
        if g + 2 >= heads:
            every_owner(lambda r, zz: across(g, r, zz).wait_send())
        every_owner(lambda r, zz: share(g, r, zz, c).wait_send())
        every_owner(lambda r, zz: share_far(g, r, zz, c).wait_send())
        for p in range(2):
            for t in range(zsz - 1):
                @pl.when((z < zsz - 1) & (z - t >= 0))
                def _():
                    up(g, p, t, z - t, s + ysz).wait_send()

                @pl.when((z > 0) & (z + t <= zsz - 1))
                def _():
                    down(g, p, t, z + t, s - ysz).wait_send()

    def share_rows():
        @pl.when(z < zsz - 1)
        def _():
            row_up(0, z, s + ysz).start()

        @pl.when(z > 0)
        def _():
            row_down(0, z, s - ysz).start()

    def gather_rows(t):
        @pl.when(z - 1 - t >= 0)
        def _():
            row_up(t, z - 1 - t, s).wait_recv()
            if t + 1 < zsz - 1:
                @pl.when(z < zsz - 1)
                def _():
                    row_up(t + 1, z - 1 - t, s + ysz).start()

        @pl.when(z + 1 + t <= zsz - 1)
        def _():
            row_down(t, z + 1 + t, s).wait_recv()
            if t + 1 < zsz - 1:
                @pl.when(z > 0)
                def _():
                    row_down(t + 1, z + 1 + t, s - ysz).start()

    def drain_rows():
        row_side(y).wait_send()
        for t in range(zsz - 1):
            @pl.when((z < zsz - 1) & (z - t >= 0))
            def _():
                row_up(t, z - t, s + ysz).wait_send()

            @pl.when((z > 0) & (z + t <= zsz - 1))
            def _():
                row_down(t, z + t, s - ysz).wait_send()

    def slot_of(column, place, i):
        b = rows_s[column, place, 0, blk_seq + i]
        home = lax.div(b, blk_seq)
        slot = rows_s[lax.rem(home, ysz), lax.div(home, ysz), 0, lax.rem(b, blk_seq)]
        owner = lax.div(slot, nh)
        return lax.rem(slot, nh), lax.div(owner, ysz), lax.rem(owner, ysz)

    def plan_send():
        row_side(1 - y).wait_recv()
        table = pltpu.make_async_copy(rows_v, rows_s, local_sem)
        table.start()
        table.wait()
        first = jnp.full((1, 128), nh, jnp.int32)
        last = jnp.full((1, 128), -1, jnp.int32)
        for i in range(blk_seq * entries):
            j, oz, oy = slot_of(1 - y, z, i)
            r = jnp.where(oz < z, z - oz, jnp.where(oz > z, zsz - 1 + oz - z, 0))
            hit = lane == jnp.where(oy == y, r, -1)
            first = jnp.where(hit, jnp.minimum(first, j), first)
            last = jnp.where(hit, jnp.maximum(last, j), last)
        plan_v[0:1, :] = first
        plan_v[1:2, :] = last
        copy = pltpu.make_async_copy(plan_v, plan_s, local_sem)
        copy.start()
        copy.wait()

    def plan_fetch():
        mine = [slot_of(y, z, i) for i in range(blk_seq * entries)]
        js = jnp.zeros((1, 128), jnp.int32)
        ozs = jnp.zeros((1, 128), jnp.int32)
        oys = jnp.zeros((1, 128), jnp.int32)
        for i, (j, oz, oy) in enumerate(mine):
            js = jnp.where(lane == i, j, js)
            ozs = jnp.where(lane == i, oz, ozs)
            oys = jnp.where(lane == i, oy, oys)
        second = jnp.zeros((1, 128), jnp.int32)
        for j, oz, oy in mine:
            second = jnp.where((ozs == oz) & (oys == oy) & (js > j), 1, second)
        place = jnp.where(oys == y, ozs * nh + js, zsz * nh + ozs * PER_OWNER + second)
        place_v[0:1, :] = place
        copy = pltpu.make_async_copy(place_v, place_s, local_sem)
        copy.start()
        copy.wait()

    factor = math.log2(math.e) / math.sqrt(HEAD_SIZE)

    def fetch(g, j):
        for e in range(entries):
            place = place_s[0, j * entries + e]
            rows = slice(e * BLOCK_ROWS, (e + 1) * BLOCK_ROWS)
            kcat[rows, :] = kv[g][0, place]
            vcat[rows, :HEAD_SIZE] = kv[g][1, place]

    def bias_of(j):
        rest = lax.broadcasted_iota(jnp.int32, (1, (entries - 1) * BLOCK_ROWS), 1) + BLOCK_ROWS
        return jnp.where(rest < cnt_ref[j] * BLOCK_ROWS, 0.0, -jnp.inf).astype(jnp.float32)

    def pair(q2, bias):
        q2 = jnp.concatenate([q2[:, :HEAD_SIZE], q2[:, HEAD_SIZE:]], axis=0)
        scores = lax.dot_general(q2, kcat[...], (((1,), (1,)), ((), ())),
                                 preferred_element_type=jnp.float32)
        own = scores[:, :BLOCK_ROWS] + diag[...]
        others = scores[:, BLOCK_ROWS:] + bias
        scores = jnp.concatenate([own, others], axis=1)
        top = jnp.max(scores, axis=1, keepdims=True)
        weights = jnp.exp2((scores - top) * factor).astype(jnp.bfloat16)
        mixed = jnp.dot(weights, vcat[...], preferred_element_type=jnp.float32)
        result = (mixed[:, :HEAD_SIZE] / mixed[:, HEAD_SIZE:]).astype(jnp.bfloat16)
        return jnp.concatenate([result[:BLOCK_ROWS], result[BLOCK_ROWS:]], axis=1)

    span = 2 * HEAD_SIZE

    def result_out(g, i):
        return remote(obuf.at[g, :, pl.ds(i * span, span)],
                      out_ref.at[:, lanes((side * heads + g) * pairs + i, span)],
                      os_.at[g, i], or_.at[g, i], (s, x_peer))

    def result_in(g, i):
        return remote(obuf.at[g, :, pl.ds(i * span, span)],
                      out_ref.at[:, lanes(((1 - side) * heads + g) * pairs + i, span)],
                      os_.at[g, i], or_.at[g, i], (s, x_peer))

    share_rows()
    loads[0].wait()
    loads[1].wait()
    for g in range(heads):
        head_near(g, 1 - c, h).start()
        for role in range(2):
            head_far(g, role).start()
        kv[g][c, z * nh + h] = kvin[c, :, lanes(side * heads + g, HEAD_SIZE)]
    loads[2].wait()
    for g in range(heads):
        q_head(g).start()
    last = zsz - 2
    open_near(0)
    gather_rows(0)
    open_far(0)
    for t in range(1, zsz - 1):
        gather_rows(t)
    row_side(y).start()
    open_z(1)
    step(0, 0)
    plan_send()
    open_y(0)
    side_step(0, 0)
    for t in range(1, last):
        step(0, t)
        side_step(0, t)
    open_z(2)
    plan_fetch()

    def far_query(g):
        fetch(g, x_peer)
        bias = bias_of(x_peer)
        q_head(g).wait_recv()
        for i in range(pairs):
            obuf[g, :, i * span:(i + 1) * span] = pair(qbuf[g, :, i * span:(i + 1) * span], bias)
            if g + 1 == heads and i > 0:
                result_out(g, i - 1).start()
        for i in range(pairs - 1 if g + 1 == heads else 0, pairs):
            result_out(g, i).start()

    def own_query(g):
        fetch(g, h)
        bias = bias_of(h)
        for i in range(pairs):
            cols = lanes((side * heads + g) * pairs + i, span)
            out_ref[:, cols] = pair(qv[:, cols], bias)

    for g in range(heads):
        more = g + 1 < heads
        step(g, last)
        side_step(g, last)
        if g > 0:
            own_query(g - 1)
        if more:
            step(g + 1, 0)
            open_y(g + 1)
            side_step(g + 1, 0)
        for t in range(-1, zsz - 1):
            take_step(g, t)
        if more:
            for t in range(1, last):
                step(g + 1, t)
                side_step(g + 1, t)
            if g + 3 < heads:
                open_z(g + 3)
        close(g)
        far_query(g)
    own_query(heads - 1)

    for g in range(heads):
        drain(g)
    drain_rows()
    for g in range(heads):
        for i in range(pairs):
            result_out(g, i).wait_send()
            result_in(g, i).wait_recv()


def body(queries, keys, values, selected, counts, block_slot):
    ns = lax.axis_size("seq")
    nh = lax.axis_size("head")
    blk_seq, entries = selected.shape
    rows = queries.shape[0]
    heads = keys.shape[1] // HEAD_SIZE // 2
    width = queries.shape[1] // 2 // heads
    assert rows == BLOCK_ROWS and blk_seq == nh and nh == 4
    assert ns % Y_SIZE == 0 and ns > 2 * Y_SIZE and heads > 2
    hbm = pl.BlockSpec(memory_space=pl.ANY)
    smem = pl.BlockSpec(memory_space=pltpu.SMEM)
    zsz = ns // Y_SIZE
    dma = pltpu.SemaphoreType.DMA
    hops = max(zsz - 1, 1)
    held = zsz * (nh + PER_OWNER)
    pairs = width // (2 * HEAD_SIZE)
    big = [pltpu.with_memory_space_constraint(a, pltpu.HBM) for a in (queries, keys, values)]
    return pl.pallas_call(
        functools.partial(kernel, ns, nh, heads, entries),
        out_shape=pltpu.VMEM(queries.shape, jnp.bfloat16),
        in_specs=[hbm, hbm, hbm, smem, smem, smem],
        out_specs=pl.BlockSpec(memory_space=pltpu.VMEM),
        scratch_shapes=[
            pltpu.VMEM(queries.shape, jnp.bfloat16),
            pltpu.VMEM((2,) + keys.shape, jnp.bfloat16),
            pltpu.VMEM((heads, rows, width), jnp.bfloat16),
            pltpu.VMEM((heads, rows, width), jnp.bfloat16),
            pltpu.VMEM((entries * BLOCK_ROWS, HEAD_SIZE), jnp.bfloat16),
            pltpu.VMEM((entries * BLOCK_ROWS, 2 * HEAD_SIZE), jnp.bfloat16),
            pltpu.VMEM((2 * BLOCK_ROWS, BLOCK_ROWS), jnp.float32),
            pltpu.VMEM((2, zsz * PER_OWNER, BLOCK_ROWS, HEAD_SIZE), jnp.bfloat16),
            pltpu.VMEM((Y_SIZE, zsz, 1, 128), jnp.int32),
            pltpu.SMEM((Y_SIZE, zsz, 1, 128), jnp.int32),
            pltpu.VMEM((8, 128), jnp.int32),
            pltpu.SMEM((8, 128), jnp.int32),
            pltpu.VMEM((8, 128), jnp.int32),
            pltpu.SMEM((8, 128), jnp.int32),
            dma((3,)), dma,
            dma((heads, 3)), dma((heads, 3)),
            dma((heads,)), dma((heads,)),
            dma((heads, 2, hops)), dma((heads, 2, hops)),
            dma((heads, 2, hops)), dma((heads, 2, hops)),
            dma((heads, 2 * zsz)), dma((heads, 2 * zsz)),
            dma((heads, 2, 2 * zsz)), dma((heads, 2, 2 * zsz)),
            dma((heads, pairs)), dma((heads, pairs)),
            dma((1 + 2 * hops,)), dma((1 + 2 * hops,)),
        ] + [pltpu.VMEM((2, held, BLOCK_ROWS, HEAD_SIZE), jnp.bfloat16)] * heads,
        compiler_params=pltpu.CompilerParams(
            collective_id=0, has_side_effects=True, vmem_limit_bytes=60 * 1024 * 1024),
        name="block_attention",
    )(*big, selected, counts, block_slot)


def solution(mesh):
    return jax.shard_map(
        body,
        mesh=mesh,
        in_specs=(
            P(("seq", "head"), None),
            P(("seq", "head"), None),
            P(("seq", "head"), None),
            P("seq", None),
            P("seq"),
            P("seq"),
        ),
        out_specs=P(("seq", "head"), None),
        check_vma=False,
    )
```

```python
import functools
import math

import jax
import jax.numpy as jnp
from jax import lax
from jax.experimental import pallas as pl
from jax.experimental.pallas import tpu as pltpu
from jax.sharding import PartitionSpec as P

QUERY_HEADS = 64
KEY_VALUE_HEADS = 8
HEAD_SIZE = 128
BLOCK_ROWS = 128
Y_SIZE = 2
PER_OWNER = 2
MESH = pl.DeviceIdType.MESH


def kernel(ns, nh, heads, entries, q_hbm, k_hbm, v_hbm, sel_ref, cnt_ref, own_slot_ref, out_ref,
           qv, kvin, qbuf, obuf, kcat, vcat, diag, stage, rows_v, rows_s, plan_v, plan_s, place_v, place_s,
           ins, local_sem, hs, hr, qs, qr, us, ur, ds_, dr, ys, yr, cs, cr, os_, or_, ss, sr, *kv):
    s = lax.axis_index("seq")
    h = lax.axis_index("head")
    ysz = Y_SIZE
    zsz = ns // ysz
    hops = max(zsz - 1, 1)
    held = zsz * (nh + PER_OWNER)
    z = s // ysz
    y = s % ysz
    y_peer = s + 1 - 2 * y
    half = nh // 2
    side = h // half
    c = h % half
    partner = side * half + 1 - c
    x_peer = (1 - side) * half + c
    width = qbuf.shape[2]
    pairs = width // (2 * HEAD_SIZE)
    blk_seq = sel_ref.shape[0]

    def remote(src, dst, send, recv, dev):
        return pltpu.make_async_remote_copy(
            src_ref=src, dst_ref=dst, send_sem=send, recv_sem=recv,
            device_id=dev, device_id_type=MESH)

    def lanes(unit, size):
        return pl.ds(pl.multiple_of(unit * size, size), size)

    loads = [pltpu.make_async_copy(k_hbm, kvin.at[0], ins.at[0]),
             pltpu.make_async_copy(v_hbm, kvin.at[1], ins.at[1]),
             pltpu.make_async_copy(q_hbm, qv, ins.at[2])]
    for load in loads:
        load.start()

    barrier = pltpu.get_barrier_semaphore()
    for d in range(1, nh):
        pl.semaphore_signal(barrier, inc=1, device_id=(s, (h + d) % nh), device_id_type=MESH)
    pl.semaphore_signal(barrier, inc=1, device_id=(y_peer, h), device_id_type=MESH)

    @pl.when(z < zsz - 1)
    def _():
        pl.semaphore_signal(barrier, inc=1, device_id=(s + ysz, h), device_id_type=MESH)

    @pl.when(z > 0)
    def _():
        pl.semaphore_signal(barrier, inc=1, device_id=(s - ysz, h), device_id_type=MESH)

    lane = lax.broadcasted_iota(jnp.int32, (1, 128), 1)
    info = jnp.zeros((1, 128), jnp.int32)
    for j in range(blk_seq):
        info = jnp.where(lane == j, own_slot_ref[j], info)
        for e in range(entries):
            block = jnp.where(e < cnt_ref[j], sel_ref[j, e], sel_ref[j, 0])
            info = jnp.where(lane == blk_seq + j * entries + e, block, info)
    rows_v[y, z] = info
    pair_rows = 2 * BLOCK_ROWS
    row = lax.rem(lax.broadcasted_iota(jnp.int32, (pair_rows, BLOCK_ROWS), 0), BLOCK_ROWS)
    col = lax.broadcasted_iota(jnp.int32, (pair_rows, BLOCK_ROWS), 1)
    diag[...] = jnp.where(col <= row, 0.0, -jnp.inf).astype(jnp.float32)
    vcat[:, HEAD_SIZE:] = jnp.ones((entries * BLOCK_ROWS, HEAD_SIZE), jnp.bfloat16)

    pl.semaphore_wait(barrier, nh + jnp.where(z < zsz - 1, 1, 0) + jnp.where(z > 0, 1, 0))

    def row_side(column):
        return remote(rows_v.at[column], rows_v.at[column], ss.at[0], sr.at[0], (y_peer, h))

    def row_up(t, zz, dev):
        ref = rows_v.at[y, zz]
        return remote(ref, ref, ss.at[1 + t], sr.at[1 + t], (dev, h))

    def row_down(t, zz, dev):
        ref = rows_v.at[y, zz]
        return remote(ref, ref, ss.at[1 + hops + t], sr.at[1 + hops + t], (dev, h))

    def head_near(g, role, place):
        return remote(kvin.at[role, :, lanes(side * heads + g, HEAD_SIZE)],
                      kv[g].at[role, z * nh + place],
                      hs.at[g], hr.at[g, 0], (s, partner))

    def head_far(g, role):
        return remote(kvin.at[role, :, lanes((1 - side) * heads + g, HEAD_SIZE)],
                      kv[g].at[role, z * nh + h],
                      hs.at[g], hr.at[g, 1], (s, (1 - side) * half + role))

    def head_far_in(g):
        ref = kv[g].at[c, pl.ds(z * nh + (1 - side) * half, half)]
        return remote(ref, ref, hs.at[g], hr.at[g, 1], (s, x_peer))

    def head_sent(g):
        ref = kv[g].at[0, pl.ds(0, nh - 1)]
        return remote(ref, ref, hs.at[g], hr.at[g, 1], (s, x_peer))

    def q_head(g):
        return remote(qv.at[:, lanes((1 - side) * heads + g, width)], qbuf.at[g],
                      qs, qr.at[g], (s, x_peer))

    def part(g, zz, p):
        lo = (side + p) % 2 * half
        return kv[g].at[c, pl.ds(zz * nh + lo, half)]

    def up(g, p, t, zz, dev):
        ref = part(g, zz, p)
        return remote(ref, ref, us.at[g], ur.at[g, p, t], (dev, h))

    def down(g, p, t, zz, dev):
        ref = part(g, zz, p)
        return remote(ref, ref, ds_.at[g], dr.at[g, p, t], (dev, h))

    def ups(g, count):
        ref = kv[g].at[c, pl.ds(0, count * nh)]
        return remote(ref, ref, us.at[g], ur.at[g, 0, 0], (s, h))

    def downs(g, count):
        ref = kv[g].at[c, pl.ds((zsz - count) * nh, count * nh)]
        return remote(ref, ref, ds_.at[g], dr.at[g, 0, 0], (s, h))

    def across(g, zz, count):
        return remote(stage.at[g % 2, pl.ds(zz * PER_OWNER, count * PER_OWNER)],
                      kv[g].at[c, pl.ds(zsz * nh + zz * PER_OWNER, count * PER_OWNER)],
                      ys.at[g], yr.at[g], (y_peer, h))

    def share(g, start, size, role):
        ref = kv[g].at[role, pl.ds(start, size)]
        return remote(ref, ref, cs.at[g], cr.at[g], (s, partner))

    def pass_on(g, r, zz):
        for k in range(PER_OWNER):
            pick = plan_s[k, r]
            chosen = kv[g][c, zz * nh + nh - 1]
            for j in reversed(range(nh - 1)):
                chosen = jnp.where(pick == j, kv[g][c, zz * nh + j], chosen)
            stage[g % 2, zz * PER_OWNER + k] = chosen
        across(g, zz, 1).start()
        share(g, zz * nh, nh, c).start()

    def take_far(g):
        across(g, 0, zsz).wait_recv()
        share(g, zsz * nh, zsz * PER_OWNER, c).start()

    def owners(t, call):
        @pl.when(z - 1 - t >= 0)
        def _():
            call(1 + t, z - 1 - t)

        @pl.when(z + 1 + t <= zsz - 1)
        def _():
            call(zsz + t, z + 1 + t)

    def send_both(g, p):
        if zsz > 1:
            @pl.when(z < zsz - 1)
            def _():
                up(g, p, 0, z, s + ysz).start()

            @pl.when(z > 0)
            def _():
                down(g, p, 0, z, s - ysz).start()

    def open_near(g):
        head_near(g, c, partner).wait_recv()
        send_both(g, 0)

    def open_far(g):
        head_far_in(g).wait_recv()
        send_both(g, 1)

    def open_z(g):
        open_near(g)
        open_far(g)

    def open_y(g):
        if g >= 2:
            across(g - 2, 0, zsz).wait_send()
        pass_on(g, 0, z)

    def step(g, t):
        for p in range(2):
            @pl.when(z - 1 - t >= 0)
            def _():
                up(g, p, t, z - 1 - t, s).wait_recv()
                if t + 1 < zsz - 1:
                    @pl.when(z < zsz - 1)
                    def _():
                        up(g, p, t + 1, z - 1 - t, s + ysz).start()

            @pl.when(z + 1 + t <= zsz - 1)
            def _():
                down(g, p, t, z + 1 + t, s).wait_recv()
                if t + 1 < zsz - 1:
                    @pl.when(z > 0)
                    def _():
                        down(g, p, t + 1, z + 1 + t, s - ysz).start()

    def side_step(g, t):
        owners(t, lambda r, zz: pass_on(g, r, zz))

    def close(g):
        share(g, 0, held, 1 - c).wait_recv()

    def drain(g):
        head_sent(g).wait_send()
        if g + 2 >= heads:
            across(g, 0, zsz).wait_send()
        share(g, 0, held, c).wait_send()
        for count in range(1, zsz):
            @pl.when(z == count - 1)
            def _():
                ups(g, count).wait_send()

            @pl.when(z == zsz - count)
            def _():
                downs(g, count).wait_send()

    def share_rows():
        @pl.when(z < zsz - 1)
        def _():
            row_up(0, z, s + ysz).start()

        @pl.when(z > 0)
        def _():
            row_down(0, z, s - ysz).start()

    def gather_rows(t):
        @pl.when(z - 1 - t >= 0)
        def _():
            row_up(t, z - 1 - t, s).wait_recv()
            if t + 1 < zsz - 1:
                @pl.when(z < zsz - 1)
                def _():
                    row_up(t + 1, z - 1 - t, s + ysz).start()

        @pl.when(z + 1 + t <= zsz - 1)
        def _():
            row_down(t, z + 1 + t, s).wait_recv()
            if t + 1 < zsz - 1:
                @pl.when(z > 0)
                def _():
                    row_down(t + 1, z + 1 + t, s - ysz).start()

    def drain_rows():
        row_side(y).wait_send()
        for t in range(zsz - 1):
            @pl.when((z < zsz - 1) & (z - t >= 0))
            def _():
                row_up(t, z - t, s + ysz).wait_send()

            @pl.when((z > 0) & (z + t <= zsz - 1))
            def _():
                row_down(t, z + t, s - ysz).wait_send()

    def slot_of(column, place, i):
        b = rows_s[column, place, 0, blk_seq + i]
        home = lax.div(b, blk_seq)
        slot = rows_s[lax.rem(home, ysz), lax.div(home, ysz), 0, lax.rem(b, blk_seq)]
        owner = lax.div(slot, nh)
        return lax.rem(slot, nh), lax.div(owner, ysz), lax.rem(owner, ysz)

    def plan_send():
        row_side(1 - y).wait_recv()
        table = pltpu.make_async_copy(rows_v, rows_s, local_sem)
        table.start()
        table.wait()
        first = jnp.full((1, 128), nh, jnp.int32)
        last = jnp.full((1, 128), -1, jnp.int32)
        for i in range(blk_seq * entries):
            j, oz, oy = slot_of(1 - y, z, i)
            r = jnp.where(oz < z, z - oz, jnp.where(oz > z, zsz - 1 + oz - z, 0))
            hit = lane == jnp.where(oy == y, r, -1)
            first = jnp.where(hit, jnp.minimum(first, j), first)
            last = jnp.where(hit, jnp.maximum(last, j), last)
        plan_v[0:1, :] = first
        plan_v[1:2, :] = last
        copy = pltpu.make_async_copy(plan_v, plan_s, local_sem)
        copy.start()
        copy.wait()

    def plan_fetch():
        mine = [slot_of(y, z, i) for i in range(blk_seq * entries)]
        js = jnp.zeros((1, 128), jnp.int32)
        ozs = jnp.zeros((1, 128), jnp.int32)
        oys = jnp.zeros((1, 128), jnp.int32)
        for i, (j, oz, oy) in enumerate(mine):
            js = jnp.where(lane == i, j, js)
            ozs = jnp.where(lane == i, oz, ozs)
            oys = jnp.where(lane == i, oy, oys)
        second = jnp.zeros((1, 128), jnp.int32)
        for j, oz, oy in mine:
            second = jnp.where((ozs == oz) & (oys == oy) & (js > j), 1, second)
        place = jnp.where(oys == y, ozs * nh + js, zsz * nh + ozs * PER_OWNER + second)
        place_v[0:1, :] = place
        copy = pltpu.make_async_copy(place_v, place_s, local_sem)
        copy.start()
        copy.wait()

    factor = math.log2(math.e) / math.sqrt(HEAD_SIZE)

    def fetch(g, j):
        for e in range(entries):
            place = place_s[0, j * entries + e]
            rows = slice(e * BLOCK_ROWS, (e + 1) * BLOCK_ROWS)
            kcat[rows, :] = kv[g][0, place]
            vcat[rows, :HEAD_SIZE] = kv[g][1, place]

    def bias_of(j):
        rest = lax.broadcasted_iota(jnp.int32, (1, (entries - 1) * BLOCK_ROWS), 1) + BLOCK_ROWS
        return jnp.where(rest < cnt_ref[j] * BLOCK_ROWS, 0.0, -jnp.inf).astype(jnp.float32)

    def pair(q2, bias):
        q2 = jnp.concatenate([q2[:, :HEAD_SIZE], q2[:, HEAD_SIZE:]], axis=0)
        scores = lax.dot_general(q2, kcat[...], (((1,), (1,)), ((), ())),
                                 preferred_element_type=jnp.float32)
        own = scores[:, :BLOCK_ROWS] + diag[...]
        others = scores[:, BLOCK_ROWS:] + bias
        scores = jnp.concatenate([own, others], axis=1)
        top = jnp.max(scores, axis=1, keepdims=True)
        weights = jnp.exp2((scores - top) * factor).astype(jnp.bfloat16)
        mixed = jnp.dot(weights, vcat[...], preferred_element_type=jnp.float32)
        result = (mixed[:, :HEAD_SIZE] / mixed[:, HEAD_SIZE:]).astype(jnp.bfloat16)
        return jnp.concatenate([result[:BLOCK_ROWS], result[BLOCK_ROWS:]], axis=1)

    span = 2 * HEAD_SIZE

    def result_out(g, i, size):
        cols = pl.ds((side * heads + g) * width + i * size, size)
        cols = pl.ds(pl.multiple_of(cols.start, size), size)
        return remote(obuf.at[g, :, pl.ds(i * size, size)], out_ref.at[:, cols],
                      os_, or_, (s, x_peer))

    def results():
        cols = lanes(1 - side, heads * width)
        return remote(qv.at[:, cols], out_ref.at[:, cols], os_, or_, (s, x_peer))

    share_rows()
    loads[0].wait()
    loads[1].wait()
    for g in range(heads):
        head_near(g, 1 - c, h).start()
        for role in range(2):
            head_far(g, role).start()
        kv[g][c, z * nh + h] = kvin[c, :, lanes(side * heads + g, HEAD_SIZE)]
    loads[2].wait()
    for g in range(heads):
        q_head(g).start()
    last = zsz - 2
    open_near(0)
    gather_rows(0)
    open_near(1)
    open_far(0)
    for t in range(1, zsz - 1):
        gather_rows(t)
    row_side(y).start()
    open_far(1)
    step(0, 0)
    open_z(2)
    plan_send()
    open_y(0)
    side_step(0, 0)
    for t in range(1, last):
        step(0, t)
        side_step(0, t)
    plan_fetch()

    def far_query(g):
        fetch(g, x_peer)
        bias = bias_of(x_peer)
        q_head(g).wait_recv()
        for i in range(pairs):
            obuf[g, :, i * span:(i + 1) * span] = pair(qbuf[g, :, i * span:(i + 1) * span], bias)
            if g + 1 == heads and i > 0:
                result_out(g, i - 1, span).start()
        if g + 1 == heads:
            result_out(g, pairs - 1, span).start()
        else:
            result_out(g, 0, width).start()

    def own_query(g):
        fetch(g, h)
        bias = bias_of(h)
        for i in range(pairs):
            cols = lanes((side * heads + g) * pairs + i, span)
            out_ref[:, cols] = pair(qv[:, cols], bias)

    for g in range(heads):
        more = g + 1 < heads
        step(g, last)
        side_step(g, last)
        if g > 0:
            own_query(g - 1)
        if g + 3 < heads:
            open_z(g + 3)
        if more:
            step(g + 1, 0)
            open_y(g + 1)
            side_step(g + 1, 0)
        take_far(g)
        if more:
            for t in range(1, last):
                step(g + 1, t)
                side_step(g + 1, t)
        close(g)
        far_query(g)
    own_query(heads - 1)

    for g in range(heads):
        drain(g)
    drain_rows()
    remote(qbuf, qbuf, qs, qr.at[0], (s, x_peer)).wait_send()
    results().wait_send()
    results().wait_recv()


def body(queries, keys, values, selected, counts, block_slot):
    ns = lax.axis_size("seq")
    nh = lax.axis_size("head")
    blk_seq, entries = selected.shape
    rows = queries.shape[0]
    heads = keys.shape[1] // HEAD_SIZE // 2
    width = queries.shape[1] // 2 // heads
    assert rows == BLOCK_ROWS and blk_seq == nh and nh == 4
    assert ns % Y_SIZE == 0 and ns > 2 * Y_SIZE and heads > 2
    hbm = pl.BlockSpec(memory_space=pl.ANY)
    smem = pl.BlockSpec(memory_space=pltpu.SMEM)
    zsz = ns // Y_SIZE
    dma = pltpu.SemaphoreType.DMA
    hops = max(zsz - 1, 1)
    held = zsz * (nh + PER_OWNER)
    big = [pltpu.with_memory_space_constraint(a, pltpu.HBM) for a in (queries, keys, values)]
    return pl.pallas_call(
        functools.partial(kernel, ns, nh, heads, entries),
        out_shape=pltpu.VMEM(queries.shape, jnp.bfloat16),
        in_specs=[hbm, hbm, hbm, smem, smem, smem],
        out_specs=pl.BlockSpec(memory_space=pltpu.VMEM),
        scratch_shapes=[
            pltpu.VMEM(queries.shape, jnp.bfloat16),
            pltpu.VMEM((2,) + keys.shape, jnp.bfloat16),
            pltpu.VMEM((heads, rows, width), jnp.bfloat16),
            pltpu.VMEM((heads, rows, width), jnp.bfloat16),
            pltpu.VMEM((entries * BLOCK_ROWS, HEAD_SIZE), jnp.bfloat16),
            pltpu.VMEM((entries * BLOCK_ROWS, 2 * HEAD_SIZE), jnp.bfloat16),
            pltpu.VMEM((2 * BLOCK_ROWS, BLOCK_ROWS), jnp.float32),
            pltpu.VMEM((2, zsz * PER_OWNER, BLOCK_ROWS, HEAD_SIZE), jnp.bfloat16),
            pltpu.VMEM((Y_SIZE, zsz, 1, 128), jnp.int32),
            pltpu.SMEM((Y_SIZE, zsz, 1, 128), jnp.int32),
            pltpu.VMEM((8, 128), jnp.int32),
            pltpu.SMEM((8, 128), jnp.int32),
            pltpu.VMEM((8, 128), jnp.int32),
            pltpu.SMEM((8, 128), jnp.int32),
            dma((3,)), dma,
            dma((heads,)), dma((heads, 2)),
            dma, dma((heads,)),
            dma((heads,)), dma((heads, 2, hops)),
            dma((heads,)), dma((heads, 2, hops)),
            dma((heads,)), dma((heads,)),
            dma((heads,)), dma((heads,)),
            dma, dma,
            dma((1 + 2 * hops,)), dma((1 + 2 * hops,)),
        ] + [pltpu.VMEM((2, held, BLOCK_ROWS, HEAD_SIZE), jnp.bfloat16)] * heads,
        compiler_params=pltpu.CompilerParams(
            collective_id=0, has_side_effects=True, vmem_limit_bytes=60 * 1024 * 1024),
        name="block_attention",
    )(*big, selected, counts, block_slot)


def solution(mesh):
    return jax.shard_map(
        body,
        mesh=mesh,
        in_specs=(
            P(("seq", "head"), None),
            P(("seq", "head"), None),
            P(("seq", "head"), None),
            P("seq", None),
            P("seq"),
            P("seq"),
        ),
        out_specs=P(("seq", "head"), None),
        check_vma=False,
    )
```

```python
import functools
import math

import jax
import jax.numpy as jnp
from jax import lax
from jax.experimental import pallas as pl
from jax.experimental.pallas import tpu as pltpu
from jax.sharding import PartitionSpec as P

QUERY_HEADS = 64
KEY_VALUE_HEADS = 8
HEAD_SIZE = 128
BLOCK_ROWS = 128
Y_SIZE = 2
PER_OWNER = 2
MESH = pl.DeviceIdType.MESH


def kernel(ns, nh, heads, entries, q_hbm, k_hbm, v_hbm, sel_hbm, cnt_hbm, slot_hbm, out_ref,
           sel_ref, cnt_ref, own_slot_ref,
           qv, kvin, qbuf, obuf, kcat, vcat, diag, stage, rows_v, rows_s, plan_v, plan_s, place_v, place_s,
           ins, local_sem, hs, hr, qs, qr, us, ur, ds_, dr, ys, yr, cs, cr, os_, or_, ss, sr, *kv):
    s = lax.axis_index("seq")
    h = lax.axis_index("head")
    ysz = Y_SIZE
    zsz = ns // ysz
    hops = max(zsz - 1, 1)
    held = zsz * (nh + PER_OWNER)
    z = s // ysz
    y = s % ysz
    y_peer = s + 1 - 2 * y
    half = nh // 2
    side = h // half
    c = h % half
    partner = side * half + 1 - c
    x_peer = (1 - side) * half + c
    width = qbuf.shape[2]
    pairs = width // (2 * HEAD_SIZE)
    blk_seq = sel_ref.shape[0]

    def remote(src, dst, send, recv, dev):
        return pltpu.make_async_remote_copy(
            src_ref=src, dst_ref=dst, send_sem=send, recv_sem=recv,
            device_id=dev, device_id_type=MESH)

    def lanes(unit, size):
        return pl.ds(pl.multiple_of(unit * size, size), size)

    barrier = pltpu.get_barrier_semaphore()
    for d in range(1, nh):
        pl.semaphore_signal(barrier, inc=1, device_id=(s, (h + d) % nh), device_id_type=MESH)
    pl.semaphore_signal(barrier, inc=1, device_id=(y_peer, h), device_id_type=MESH)

    @pl.when(z < zsz - 1)
    def _():
        pl.semaphore_signal(barrier, inc=1, device_id=(s + ysz, h), device_id_type=MESH)

    @pl.when(z > 0)
    def _():
        pl.semaphore_signal(barrier, inc=1, device_id=(s - ysz, h), device_id_type=MESH)

    loads = [pltpu.make_async_copy(sel_hbm, sel_ref, ins.at[3]),
             pltpu.make_async_copy(cnt_hbm, cnt_ref, ins.at[4]),
             pltpu.make_async_copy(slot_hbm, own_slot_ref, ins.at[5]),
             pltpu.make_async_copy(k_hbm, kvin.at[0], ins.at[0]),
             pltpu.make_async_copy(v_hbm, kvin.at[1], ins.at[1]),
             pltpu.make_async_copy(q_hbm, qv, ins.at[2])]
    for load in loads:
        load.start()

    lane = lax.broadcasted_iota(jnp.int32, (1, 128), 1)
    pair_rows = 2 * BLOCK_ROWS
    row = lax.rem(lax.broadcasted_iota(jnp.int32, (pair_rows, BLOCK_ROWS), 0), BLOCK_ROWS)
    col = lax.broadcasted_iota(jnp.int32, (pair_rows, BLOCK_ROWS), 1)
    diag[...] = jnp.where(col <= row, 0.0, -jnp.inf).astype(jnp.float32)
    vcat[:, HEAD_SIZE:] = jnp.ones((entries * BLOCK_ROWS, HEAD_SIZE), jnp.bfloat16)
    for load in loads[:3]:
        load.wait()
    info = jnp.zeros((1, 128), jnp.int32)
    for j in range(blk_seq):
        info = jnp.where(lane == j, own_slot_ref[j], info)
        for e in range(entries):
            block = jnp.where(e < cnt_ref[j], sel_ref[j, e], sel_ref[j, 0])
            info = jnp.where(lane == blk_seq + j * entries + e, block, info)
    rows_v[y, z] = info

    pl.semaphore_wait(barrier, nh + jnp.where(z < zsz - 1, 1, 0) + jnp.where(z > 0, 1, 0))

    def row_side(column):
        return remote(rows_v.at[column], rows_v.at[column], ss.at[0], sr.at[0], (y_peer, h))

    def row_up(t, zz, dev):
        ref = rows_v.at[y, zz]
        return remote(ref, ref, ss.at[1 + t], sr.at[1 + t], (dev, h))

    def row_down(t, zz, dev):
        ref = rows_v.at[y, zz]
        return remote(ref, ref, ss.at[1 + hops + t], sr.at[1 + hops + t], (dev, h))

    def head_near(g, role, place):
        return remote(kvin.at[role, :, lanes(side * heads + g, HEAD_SIZE)],
                      kv[g].at[role, z * nh + place],
                      hs.at[g], hr.at[g, 0], (s, partner))

    def head_far(g, role):
        return remote(kvin.at[role, :, lanes((1 - side) * heads + g, HEAD_SIZE)],
                      kv[g].at[role, z * nh + h],
                      hs.at[g], hr.at[g, 1], (s, (1 - side) * half + role))

    def head_far_in(g):
        ref = kv[g].at[c, pl.ds(z * nh + (1 - side) * half, half)]
        return remote(ref, ref, hs.at[g], hr.at[g, 1], (s, x_peer))

    def head_sent(g):
        ref = kv[g].at[0, pl.ds(0, nh - 1)]
        return remote(ref, ref, hs.at[g], hr.at[g, 1], (s, x_peer))

    def q_head(g):
        return remote(qv.at[:, lanes((1 - side) * heads + g, width)], qbuf.at[g],
                      qs, qr.at[g], (s, x_peer))

    def part(g, zz, p):
        lo = (side + p) % 2 * half
        return kv[g].at[c, pl.ds(zz * nh + lo, half)]

    def up(g, p, t, zz, dev):
        ref = part(g, zz, p)
        return remote(ref, ref, us.at[g], ur.at[g, p, t], (dev, h))

    def down(g, p, t, zz, dev):
        ref = part(g, zz, p)
        return remote(ref, ref, ds_.at[g], dr.at[g, p, t], (dev, h))

    def ups(g, count):
        ref = kv[g].at[c, pl.ds(0, count * nh)]
        return remote(ref, ref, us.at[g], ur.at[g, 0, 0], (s, h))

    def downs(g, count):
        ref = kv[g].at[c, pl.ds((zsz - count) * nh, count * nh)]
        return remote(ref, ref, ds_.at[g], dr.at[g, 0, 0], (s, h))

    def across(g, zz, count):
        return remote(stage.at[g % 2, pl.ds(zz * PER_OWNER, count * PER_OWNER)],
                      kv[g].at[c, pl.ds(zsz * nh + zz * PER_OWNER, count * PER_OWNER)],
                      ys.at[g], yr.at[g], (y_peer, h))

    def share(g, start, size, role):
        ref = kv[g].at[role, pl.ds(start, size)]
        return remote(ref, ref, cs.at[g], cr.at[g], (s, partner))

    def pass_on(g, r, zz):
        for k in range(PER_OWNER):
            pick = plan_s[k, r]
            chosen = kv[g][c, zz * nh + nh - 1]
            for j in reversed(range(nh - 1)):
                chosen = jnp.where(pick == j, kv[g][c, zz * nh + j], chosen)
            stage[g % 2, zz * PER_OWNER + k] = chosen
        across(g, zz, 1).start()
        share(g, zz * nh, nh, c).start()

    def take_far(g):
        across(g, 0, zsz).wait_recv()
        share(g, zsz * nh, zsz * PER_OWNER, c).start()

    def owners(t, call):
        @pl.when(z - 1 - t >= 0)
        def _():
            call(1 + t, z - 1 - t)

        @pl.when(z + 1 + t <= zsz - 1)
        def _():
            call(zsz + t, z + 1 + t)

    def send_both(g, p):
        if zsz > 1:
            @pl.when(z < zsz - 1)
            def _():
                up(g, p, 0, z, s + ysz).start()

            @pl.when(z > 0)
            def _():
                down(g, p, 0, z, s - ysz).start()

    def open_near(g):
        head_near(g, c, partner).wait_recv()
        send_both(g, 0)

    def open_far(g):
        head_far_in(g).wait_recv()
        send_both(g, 1)

    def open_z(g):
        open_near(g)
        open_far(g)

    def open_y(g):
        if g >= 2:
            across(g - 2, 0, zsz).wait_send()
        pass_on(g, 0, z)

    def step(g, t):
        for p in range(2):
            @pl.when(z - 1 - t >= 0)
            def _():
                up(g, p, t, z - 1 - t, s).wait_recv()
                if t + 1 < zsz - 1:
                    @pl.when(z < zsz - 1)
                    def _():
                        up(g, p, t + 1, z - 1 - t, s + ysz).start()

            @pl.when(z + 1 + t <= zsz - 1)
            def _():
                down(g, p, t, z + 1 + t, s).wait_recv()
                if t + 1 < zsz - 1:
                    @pl.when(z > 0)
                    def _():
                        down(g, p, t + 1, z + 1 + t, s - ysz).start()

    def side_step(g, t):
        owners(t, lambda r, zz: pass_on(g, r, zz))

    def close(g):
        share(g, 0, held, 1 - c).wait_recv()

    def drain(g):
        head_sent(g).wait_send()
        if g + 2 >= heads:
            across(g, 0, zsz).wait_send()
        share(g, 0, held, c).wait_send()
        for count in range(1, zsz):
            @pl.when(z == count - 1)
            def _():
                ups(g, count).wait_send()

            @pl.when(z == zsz - count)
            def _():
                downs(g, count).wait_send()

    def share_rows():
        @pl.when(z < zsz - 1)
        def _():
            row_up(0, z, s + ysz).start()

        @pl.when(z > 0)
        def _():
            row_down(0, z, s - ysz).start()

    def gather_rows(t):
        @pl.when(z - 1 - t >= 0)
        def _():
            row_up(t, z - 1 - t, s).wait_recv()
            if t + 1 < zsz - 1:
                @pl.when(z < zsz - 1)
                def _():
                    row_up(t + 1, z - 1 - t, s + ysz).start()

        @pl.when(z + 1 + t <= zsz - 1)
        def _():
            row_down(t, z + 1 + t, s).wait_recv()
            if t + 1 < zsz - 1:
                @pl.when(z > 0)
                def _():
                    row_down(t + 1, z + 1 + t, s - ysz).start()

    def drain_rows():
        row_side(y).wait_send()
        for t in range(zsz - 1):
            @pl.when((z < zsz - 1) & (z - t >= 0))
            def _():
                row_up(t, z - t, s + ysz).wait_send()

            @pl.when((z > 0) & (z + t <= zsz - 1))
            def _():
                row_down(t, z + t, s - ysz).wait_send()

    def slot_of(column, place, i):
        b = rows_s[column, place, 0, blk_seq + i]
        home = lax.div(b, blk_seq)
        slot = rows_s[lax.rem(home, ysz), lax.div(home, ysz), 0, lax.rem(b, blk_seq)]
        owner = lax.div(slot, nh)
        return lax.rem(slot, nh), lax.div(owner, ysz), lax.rem(owner, ysz)

    def plan_send():
        row_side(1 - y).wait_recv()
        table = pltpu.make_async_copy(rows_v, rows_s, local_sem)
        table.start()
        table.wait()
        first = jnp.full((1, 128), nh, jnp.int32)
        last = jnp.full((1, 128), -1, jnp.int32)
        for i in range(blk_seq * entries):
            j, oz, oy = slot_of(1 - y, z, i)
            r = jnp.where(oz < z, z - oz, jnp.where(oz > z, zsz - 1 + oz - z, 0))
            hit = lane == jnp.where(oy == y, r, -1)
            first = jnp.where(hit, jnp.minimum(first, j), first)
            last = jnp.where(hit, jnp.maximum(last, j), last)
        plan_v[0:1, :] = first
        plan_v[1:2, :] = last
        copy = pltpu.make_async_copy(plan_v, plan_s, local_sem)
        copy.start()
        copy.wait()

    def plan_fetch():
        mine = [slot_of(y, z, i) for i in range(blk_seq * entries)]
        js = jnp.zeros((1, 128), jnp.int32)
        ozs = jnp.zeros((1, 128), jnp.int32)
        oys = jnp.zeros((1, 128), jnp.int32)
        for i, (j, oz, oy) in enumerate(mine):
            js = jnp.where(lane == i, j, js)
            ozs = jnp.where(lane == i, oz, ozs)
            oys = jnp.where(lane == i, oy, oys)
        second = jnp.zeros((1, 128), jnp.int32)
        for j, oz, oy in mine:
            second = jnp.where((ozs == oz) & (oys == oy) & (js > j), 1, second)
        place = jnp.where(oys == y, ozs * nh + js, zsz * nh + ozs * PER_OWNER + second)
        place_v[0:1, :] = place
        copy = pltpu.make_async_copy(place_v, place_s, local_sem)
        copy.start()
        copy.wait()

    factor = math.log2(math.e) / math.sqrt(HEAD_SIZE)

    def fetch(g, j):
        for e in range(entries):
            place = place_s[0, j * entries + e]
            rows = slice(e * BLOCK_ROWS, (e + 1) * BLOCK_ROWS)
            kcat[rows, :] = kv[g][0, place]
            vcat[rows, :HEAD_SIZE] = kv[g][1, place]

    def bias_of(j):
        rest = lax.broadcasted_iota(jnp.int32, (1, (entries - 1) * BLOCK_ROWS), 1) + BLOCK_ROWS
        return jnp.where(rest < cnt_ref[j] * BLOCK_ROWS, 0.0, -jnp.inf).astype(jnp.float32)

    def pair(q2, bias):
        q2 = jnp.concatenate([q2[:, :HEAD_SIZE], q2[:, HEAD_SIZE:]], axis=0)
        scores = lax.dot_general(q2, kcat[...], (((1,), (1,)), ((), ())),
                                 preferred_element_type=jnp.float32)
        own = scores[:, :BLOCK_ROWS] + diag[...]
        others = scores[:, BLOCK_ROWS:] + bias
        scores = jnp.concatenate([own, others], axis=1)
        top = jnp.max(scores, axis=1, keepdims=True)
        weights = jnp.exp2((scores - top) * factor).astype(jnp.bfloat16)
        mixed = jnp.dot(weights, vcat[...], preferred_element_type=jnp.float32)
        result = (mixed[:, :HEAD_SIZE] / mixed[:, HEAD_SIZE:]).astype(jnp.bfloat16)
        return jnp.concatenate([result[:BLOCK_ROWS], result[BLOCK_ROWS:]], axis=1)

    span = 2 * HEAD_SIZE

    def result_out(g, i, size):
        cols = pl.ds((side * heads + g) * width + i * size, size)
        cols = pl.ds(pl.multiple_of(cols.start, size), size)
        return remote(obuf.at[g, :, pl.ds(i * size, size)], out_ref.at[:, cols],
                      os_, or_, (s, x_peer))

    def results():
        cols = lanes(1 - side, heads * width)
        return remote(qv.at[:, cols], out_ref.at[:, cols], os_, or_, (s, x_peer))

    share_rows()
    loads[3].wait()
    loads[4].wait()
    for g in range(heads):
        head_near(g, 1 - c, h).start()
        for role in range(2):
            head_far(g, role).start()
        kv[g][c, z * nh + h] = kvin[c, :, lanes(side * heads + g, HEAD_SIZE)]
    loads[5].wait()
    for g in range(heads):
        q_head(g).start()
    last = zsz - 2
    open_near(0)
    gather_rows(0)
    open_near(1)
    open_near(2)
    open_far(0)
    for t in range(1, zsz - 1):
        gather_rows(t)
    row_side(y).start()
    open_far(1)
    step(0, 0)
    open_far(2)
    plan_send()
    open_y(0)
    side_step(0, 0)
    for t in range(1, last):
        step(0, t)
        side_step(0, t)
    plan_fetch()

    def far_query(g):
        fetch(g, x_peer)
        bias = bias_of(x_peer)
        q_head(g).wait_recv()
        for i in range(pairs):
            obuf[g, :, i * span:(i + 1) * span] = pair(qbuf[g, :, i * span:(i + 1) * span], bias)
            if g + 1 == heads and i == pairs // 2:
                result_out(g, 0, width // 2).start()
        if g + 1 == heads:
            result_out(g, 1, width // 2).start()
        else:
            result_out(g, 0, width).start()

    def own_query(g):
        fetch(g, h)
        bias = bias_of(h)
        for i in range(pairs):
            cols = lanes((side * heads + g) * pairs + i, span)
            out_ref[:, cols] = pair(qv[:, cols], bias)

    for g in range(heads):
        more = g + 1 < heads
        step(g, last)
        side_step(g, last)
        if g + 3 < heads:
            open_z(g + 3)
        if more:
            step(g + 1, 0)
        if g > 0:
            own_query(g - 1)
        if more:
            open_y(g + 1)
            side_step(g + 1, 0)
        take_far(g)
        if more:
            for t in range(1, last):
                step(g + 1, t)
                side_step(g + 1, t)
        close(g)
        far_query(g)
    own_query(heads - 1)

    for g in range(heads):
        drain(g)
    drain_rows()
    remote(qbuf, qbuf, qs, qr.at[0], (s, x_peer)).wait_send()
    results().wait_send()
    results().wait_recv()


def body(queries, keys, values, selected, counts, block_slot):
    ns = lax.axis_size("seq")
    nh = lax.axis_size("head")
    blk_seq, entries = selected.shape
    rows = queries.shape[0]
    heads = keys.shape[1] // HEAD_SIZE // 2
    width = queries.shape[1] // 2 // heads
    assert rows == BLOCK_ROWS and blk_seq == nh and nh == 4
    assert ns % Y_SIZE == 0 and ns > 2 * Y_SIZE and heads > 2
    hbm = pl.BlockSpec(memory_space=pl.ANY)
    zsz = ns // Y_SIZE
    dma = pltpu.SemaphoreType.DMA
    hops = max(zsz - 1, 1)
    held = zsz * (nh + PER_OWNER)
    big = [pltpu.with_memory_space_constraint(a, pltpu.HBM)
           for a in (queries, keys, values, selected, counts, block_slot)]
    return pl.pallas_call(
        functools.partial(kernel, ns, nh, heads, entries),
        out_shape=pltpu.VMEM(queries.shape, jnp.bfloat16),
        in_specs=[hbm] * 6,
        out_specs=pl.BlockSpec(memory_space=pltpu.VMEM),
        scratch_shapes=[
            pltpu.SMEM(selected.shape, jnp.int32),
            pltpu.SMEM(counts.shape, jnp.int32),
            pltpu.SMEM(block_slot.shape, jnp.int32),
            pltpu.VMEM(queries.shape, jnp.bfloat16),
            pltpu.VMEM((2,) + keys.shape, jnp.bfloat16),
            pltpu.VMEM((heads, rows, width), jnp.bfloat16),
            pltpu.VMEM((heads, rows, width), jnp.bfloat16),
            pltpu.VMEM((entries * BLOCK_ROWS, HEAD_SIZE), jnp.bfloat16),
            pltpu.VMEM((entries * BLOCK_ROWS, 2 * HEAD_SIZE), jnp.bfloat16),
            pltpu.VMEM((2 * BLOCK_ROWS, BLOCK_ROWS), jnp.float32),
            pltpu.VMEM((2, zsz * PER_OWNER, BLOCK_ROWS, HEAD_SIZE), jnp.bfloat16),
            pltpu.VMEM((Y_SIZE, zsz, 1, 128), jnp.int32),
            pltpu.SMEM((Y_SIZE, zsz, 1, 128), jnp.int32),
            pltpu.VMEM((8, 128), jnp.int32),
            pltpu.SMEM((8, 128), jnp.int32),
            pltpu.VMEM((8, 128), jnp.int32),
            pltpu.SMEM((8, 128), jnp.int32),
            dma((6,)), dma,
            dma((heads,)), dma((heads, 2)),
            dma, dma((heads,)),
            dma((heads,)), dma((heads, 2, hops)),
            dma((heads,)), dma((heads, 2, hops)),
            dma((heads,)), dma((heads,)),
            dma((heads,)), dma((heads,)),
            dma, dma,
            dma((1 + 2 * hops,)), dma((1 + 2 * hops,)),
        ] + [pltpu.VMEM((2, held, BLOCK_ROWS, HEAD_SIZE), jnp.bfloat16)] * heads,
        compiler_params=pltpu.CompilerParams(
            collective_id=0, has_side_effects=True, vmem_limit_bytes=60 * 1024 * 1024),
        name="block_attention",
    )(*big)


def solution(mesh):
    return jax.shard_map(
        body,
        mesh=mesh,
        in_specs=(
            P(("seq", "head"), None),
            P(("seq", "head"), None),
            P(("seq", "head"), None),
            P("seq", None),
            P("seq"),
            P("seq"),
        ),
        out_specs=P(("seq", "head"), None),
        check_vma=False,
    )
```

```python
import functools
import math

import jax
import jax.numpy as jnp
from jax import lax
from jax.experimental import pallas as pl
from jax.experimental.pallas import tpu as pltpu
from jax.sharding import PartitionSpec as P

QUERY_HEADS = 64
KEY_VALUE_HEADS = 8
HEAD_SIZE = 128
BLOCK_ROWS = 128
Y_SIZE = 2
PER_OWNER = 2
MESH = pl.DeviceIdType.MESH


def kernel(ns, nh, heads, entries, q_hbm, k_hbm, v_hbm, sel_hbm, cnt_hbm, slot_hbm, out_ref,
           sel_ref, cnt_ref, own_slot_ref,
           qv, kvin, qbuf, obuf, kcat, vcat, diag, stage, rows_v, rows_s, plan_v, plan_s, place_v, place_s,
           ins, local_sem, hs, hr, qs, qr, us, ur, ds_, ys, yr, cs, cr, os_, or_, ss, sr, *kv):
    s = lax.axis_index("seq")
    h = lax.axis_index("head")
    ysz = Y_SIZE
    zsz = ns // ysz
    hops = max(zsz - 1, 1)
    held = zsz * (nh + PER_OWNER)
    z = s // ysz
    y = s % ysz
    y_peer = s + 1 - 2 * y
    half = nh // 2
    side = h // half
    c = h % half
    partner = side * half + 1 - c
    x_peer = (1 - side) * half + c
    width = qbuf.shape[2]
    pairs = width // (2 * HEAD_SIZE)
    blk_seq = sel_ref.shape[0]

    def remote(src, dst, send, recv, dev):
        return pltpu.make_async_remote_copy(
            src_ref=src, dst_ref=dst, send_sem=send, recv_sem=recv,
            device_id=dev, device_id_type=MESH)

    def lanes(unit, size):
        return pl.ds(pl.multiple_of(unit * size, size), size)

    barrier = pltpu.get_barrier_semaphore()
    for d in range(1, nh):
        pl.semaphore_signal(barrier, inc=1, device_id=(s, (h + d) % nh), device_id_type=MESH)
    pl.semaphore_signal(barrier, inc=1, device_id=(y_peer, h), device_id_type=MESH)

    @pl.when(z < zsz - 1)
    def _():
        pl.semaphore_signal(barrier, inc=1, device_id=(s + ysz, h), device_id_type=MESH)

    @pl.when(z > 0)
    def _():
        pl.semaphore_signal(barrier, inc=1, device_id=(s - ysz, h), device_id_type=MESH)

    loads = [pltpu.make_async_copy(sel_hbm, sel_ref, ins.at[3]),
             pltpu.make_async_copy(cnt_hbm, cnt_ref, ins.at[4]),
             pltpu.make_async_copy(slot_hbm, own_slot_ref, ins.at[5]),
             pltpu.make_async_copy(k_hbm, kvin.at[0], ins.at[0]),
             pltpu.make_async_copy(v_hbm, kvin.at[1], ins.at[1]),
             pltpu.make_async_copy(q_hbm, qv, ins.at[2])]
    for load in loads:
        load.start()

    lane = lax.broadcasted_iota(jnp.int32, (1, 128), 1)
    pair_rows = 2 * BLOCK_ROWS
    row = lax.rem(lax.broadcasted_iota(jnp.int32, (pair_rows, BLOCK_ROWS), 0), BLOCK_ROWS)
    col = lax.broadcasted_iota(jnp.int32, (pair_rows, BLOCK_ROWS), 1)
    diag[...] = jnp.where(col <= row, 0.0, -jnp.inf).astype(jnp.float32)
    vcat[:, HEAD_SIZE:] = jnp.ones((entries * BLOCK_ROWS, HEAD_SIZE), jnp.bfloat16)
    for load in loads[:3]:
        load.wait()
    info = jnp.zeros((1, 128), jnp.int32)
    for j in range(blk_seq):
        info = jnp.where(lane == j, own_slot_ref[j], info)
        for e in range(entries):
            block = jnp.where(e < cnt_ref[j], sel_ref[j, e], sel_ref[j, 0])
            info = jnp.where(lane == blk_seq + j * entries + e, block, info)
    rows_v[y, z] = info

    pl.semaphore_wait(barrier, nh + jnp.where(z < zsz - 1, 1, 0) + jnp.where(z > 0, 1, 0))

    def row_side(column):
        return remote(rows_v.at[column], rows_v.at[column], ss.at[0], sr.at[0], (y_peer, h))

    def row_up(t, zz, dev):
        ref = rows_v.at[y, zz]
        return remote(ref, ref, ss.at[1 + t], sr.at[1 + t], (dev, h))

    def row_down(t, zz, dev):
        ref = rows_v.at[y, zz]
        return remote(ref, ref, ss.at[1 + hops + t], sr.at[1 + hops + t], (dev, h))

    def head_near(g, role, place):
        return remote(kvin.at[role, :, lanes(side * heads + g, HEAD_SIZE)],
                      kv[g].at[role, z * nh + place],
                      hs, hr.at[g, 0], (s, partner))

    def head_far(g, role):
        return remote(kvin.at[role, :, lanes((1 - side) * heads + g, HEAD_SIZE)],
                      kv[g].at[role, z * nh + h],
                      hs, hr.at[g, 1], (s, (1 - side) * half + role))

    def head_far_in(g):
        ref = kv[g].at[c, pl.ds(z * nh + (1 - side) * half, half)]
        return remote(ref, ref, hs, hr.at[g, 1], (s, x_peer))

    def head_sent():
        ref = kv[0].at[0, pl.ds(0, heads * (nh - 1))]
        return remote(ref, ref, hs, hr.at[0, 1], (s, x_peer))

    def q_head(g):
        return remote(qv.at[:, lanes((1 - side) * heads + g, width)], qbuf.at[g],
                      qs, qr.at[g], (s, x_peer))

    def part(g, zz, p):
        lo = (side + p) % 2 * half
        return kv[g].at[c, pl.ds(zz * nh + lo, half)]

    def up(g, p, t, zz, dev):
        ref = part(g, zz, p)
        return remote(ref, ref, us.at[g], ur.at[g, p, zz], (dev, h))

    def down(g, p, t, zz, dev):
        ref = part(g, zz, p)
        return remote(ref, ref, ds_.at[g], ur.at[g, p, zz], (dev, h))

    def ups(g, count):
        ref = kv[g].at[c, pl.ds(0, count * nh)]
        return remote(ref, ref, us.at[g], ur.at[g, 0, 0], (s, h))

    def downs(g, count):
        ref = kv[g].at[c, pl.ds((zsz - count) * nh, count * nh)]
        return remote(ref, ref, ds_.at[g], ur.at[g, 0, 0], (s, h))

    def across(g, zz, count):
        return remote(stage.at[g % 2, pl.ds(zz * PER_OWNER, count * PER_OWNER)],
                      kv[g].at[c, pl.ds(zsz * nh + zz * PER_OWNER, count * PER_OWNER)],
                      ys.at[g % 2], yr.at[g], (y_peer, h))

    def share(g, start, size, role):
        ref = kv[g].at[role, pl.ds(start, size)]
        return remote(ref, ref, cs.at[g], cr.at[g], (s, partner))

    def pass_on(g, r, zz):
        for k in range(PER_OWNER):
            pick = plan_s[k, r]
            chosen = kv[g][c, zz * nh + nh - 1]
            for j in reversed(range(nh - 1)):
                chosen = jnp.where(pick == j, kv[g][c, zz * nh + j], chosen)
            stage[g % 2, zz * PER_OWNER + k] = chosen
        across(g, zz, 1).start()
        share(g, zz * nh, nh, c).start()

    def take_far(g):
        across(g, 0, zsz).wait_recv()
        share(g, zsz * nh, zsz * PER_OWNER, c).start()

    def owners(t, call):
        @pl.when(z - 1 - t >= 0)
        def _():
            call(1 + t, z - 1 - t)

        @pl.when(z + 1 + t <= zsz - 1)
        def _():
            call(zsz + t, z + 1 + t)

    def send_both(g, p):
        if zsz > 1:
            @pl.when(z < zsz - 1)
            def _():
                up(g, p, 0, z, s + ysz).start()

            @pl.when(z > 0)
            def _():
                down(g, p, 0, z, s - ysz).start()

    def open_near(g):
        head_near(g, c, partner).wait_recv()
        send_both(g, 0)

    def open_far(g):
        head_far_in(g).wait_recv()
        send_both(g, 1)

    def open_z(g):
        open_near(g)
        open_far(g)

    def open_y(g):
        if g >= 2:
            across(g - 2, 0, zsz).wait_send()
        pass_on(g, 0, z)

    def step(g, t):
        for p in range(2):
            @pl.when(z - 1 - t >= 0)
            def _():
                up(g, p, t, z - 1 - t, s).wait_recv()
                if t + 1 < zsz - 1:
                    @pl.when(z < zsz - 1)
                    def _():
                        up(g, p, t + 1, z - 1 - t, s + ysz).start()

            @pl.when(z + 1 + t <= zsz - 1)
            def _():
                down(g, p, t, z + 1 + t, s).wait_recv()
                if t + 1 < zsz - 1:
                    @pl.when(z > 0)
                    def _():
                        down(g, p, t + 1, z + 1 + t, s - ysz).start()

    def side_step(g, t):
        owners(t, lambda r, zz: pass_on(g, r, zz))

    def close(g):
        share(g, 0, held, 1 - c).wait_recv()

    def drain(g):
        if g + 2 >= heads:
            across(g, 0, zsz).wait_send()
        share(g, 0, held, c).wait_send()
        for count in range(1, zsz):
            @pl.when(z == count - 1)
            def _():
                ups(g, count).wait_send()

            @pl.when(z == zsz - count)
            def _():
                downs(g, count).wait_send()

    def share_rows():
        @pl.when(z < zsz - 1)
        def _():
            row_up(0, z, s + ysz).start()

        @pl.when(z > 0)
        def _():
            row_down(0, z, s - ysz).start()

    def gather_rows(t):
        @pl.when(z - 1 - t >= 0)
        def _():
            row_up(t, z - 1 - t, s).wait_recv()
            if t + 1 < zsz - 1:
                @pl.when(z < zsz - 1)
                def _():
                    row_up(t + 1, z - 1 - t, s + ysz).start()

        @pl.when(z + 1 + t <= zsz - 1)
        def _():
            row_down(t, z + 1 + t, s).wait_recv()
            if t + 1 < zsz - 1:
                @pl.when(z > 0)
                def _():
                    row_down(t + 1, z + 1 + t, s - ysz).start()

    def drain_rows():
        row_side(y).wait_send()
        for t in range(zsz - 1):
            @pl.when((z < zsz - 1) & (z - t >= 0))
            def _():
                row_up(t, z - t, s + ysz).wait_send()

            @pl.when((z > 0) & (z + t <= zsz - 1))
            def _():
                row_down(t, z + t, s - ysz).wait_send()

    def slot_of(column, place, i):
        b = rows_s[column, place, 0, blk_seq + i]
        home = lax.div(b, blk_seq)
        slot = rows_s[lax.rem(home, ysz), lax.div(home, ysz), 0, lax.rem(b, blk_seq)]
        owner = lax.div(slot, nh)
        return lax.rem(slot, nh), lax.div(owner, ysz), lax.rem(owner, ysz)

    def plan_send():
        row_side(1 - y).wait_recv()
        table = pltpu.make_async_copy(rows_v, rows_s, local_sem)
        table.start()
        table.wait()
        first = jnp.full((1, 128), nh, jnp.int32)
        last = jnp.full((1, 128), -1, jnp.int32)
        for i in range(blk_seq * entries):
            j, oz, oy = slot_of(1 - y, z, i)
            r = jnp.where(oz < z, z - oz, jnp.where(oz > z, zsz - 1 + oz - z, 0))
            hit = lane == jnp.where(oy == y, r, -1)
            first = jnp.where(hit, jnp.minimum(first, j), first)
            last = jnp.where(hit, jnp.maximum(last, j), last)
        plan_v[0:1, :] = first
        plan_v[1:2, :] = last
        copy = pltpu.make_async_copy(plan_v, plan_s, local_sem)
        copy.start()
        copy.wait()

    def plan_fetch():
        mine = [slot_of(y, z, i) for i in range(blk_seq * entries)]
        js = jnp.zeros((1, 128), jnp.int32)
        ozs = jnp.zeros((1, 128), jnp.int32)
        oys = jnp.zeros((1, 128), jnp.int32)
        for i, (j, oz, oy) in enumerate(mine):
            js = jnp.where(lane == i, j, js)
            ozs = jnp.where(lane == i, oz, ozs)
            oys = jnp.where(lane == i, oy, oys)
        second = jnp.zeros((1, 128), jnp.int32)
        for j, oz, oy in mine:
            second = jnp.where((ozs == oz) & (oys == oy) & (js > j), 1, second)
        place = jnp.where(oys == y, ozs * nh + js, zsz * nh + ozs * PER_OWNER + second)
        place_v[0:1, :] = place
        copy = pltpu.make_async_copy(place_v, place_s, local_sem)
        copy.start()
        copy.wait()

    factor = math.log2(math.e) / math.sqrt(HEAD_SIZE)

    def fetch(g, j):
        for e in range(entries):
            place = place_s[0, j * entries + e]
            rows = slice(e * BLOCK_ROWS, (e + 1) * BLOCK_ROWS)
            kcat[rows, :] = kv[g][0, place]
            vcat[rows, :HEAD_SIZE] = kv[g][1, place]

    def bias_of(j):
        rest = lax.broadcasted_iota(jnp.int32, (1, (entries - 1) * BLOCK_ROWS), 1) + BLOCK_ROWS
        return jnp.where(rest < cnt_ref[j] * BLOCK_ROWS, 0.0, -jnp.inf).astype(jnp.float32)

    def pair(q2, bias):
        q2 = jnp.concatenate([q2[:, :HEAD_SIZE], q2[:, HEAD_SIZE:]], axis=0)
        scores = lax.dot_general(q2, kcat[...], (((1,), (1,)), ((), ())),
                                 preferred_element_type=jnp.float32)
        own = scores[:, :BLOCK_ROWS] + diag[...]
        others = scores[:, BLOCK_ROWS:] + bias
        scores = jnp.concatenate([own, others], axis=1)
        top = jnp.max(scores, axis=1, keepdims=True)
        weights = jnp.exp2((scores - top) * factor).astype(jnp.bfloat16)
        mixed = jnp.dot(weights, vcat[...], preferred_element_type=jnp.float32)
        result = (mixed[:, :HEAD_SIZE] / mixed[:, HEAD_SIZE:]).astype(jnp.bfloat16)
        return jnp.concatenate([result[:BLOCK_ROWS], result[BLOCK_ROWS:]], axis=1)

    span = 2 * HEAD_SIZE

    def result_out(g, i, size):
        cols = pl.ds((side * heads + g) * width + i * size, size)
        cols = pl.ds(pl.multiple_of(cols.start, size), size)
        return remote(obuf.at[g, :, pl.ds(i * size, size)], out_ref.at[:, cols],
                      os_, or_, (s, x_peer))

    def results():
        cols = lanes(1 - side, heads * width)
        return remote(qv.at[:, cols], out_ref.at[:, cols], os_, or_, (s, x_peer))

    share_rows()
    loads[3].wait()
    loads[4].wait()
    for g in range(heads):
        head_near(g, 1 - c, h).start()
        for role in range(2):
            head_far(g, role).start()
        kv[g][c, z * nh + h] = kvin[c, :, lanes(side * heads + g, HEAD_SIZE)]
    loads[5].wait()
    for g in range(heads):
        q_head(g).start()
    last = zsz - 2
    open_near(0)
    gather_rows(0)
    open_near(1)
    open_near(2)
    open_far(0)
    for t in range(1, zsz - 1):
        gather_rows(t)
    row_side(y).start()
    open_far(1)
    step(0, 0)
    open_far(2)
    plan_send()
    open_y(0)
    side_step(0, 0)
    for t in range(1, last):
        step(0, t)
        side_step(0, t)
    plan_fetch()

    def far_query(g):
        fetch(g, x_peer)
        bias = bias_of(x_peer)
        q_head(g).wait_recv()
        for i in range(pairs):
            obuf[g, :, i * span:(i + 1) * span] = pair(qbuf[g, :, i * span:(i + 1) * span], bias)
            if g + 1 == heads and i == pairs // 2:
                result_out(g, 0, width // 2).start()
        if g + 1 == heads:
            result_out(g, 1, width // 2).start()
        else:
            result_out(g, 0, width).start()

    def own_query(g):
        fetch(g, h)
        bias = bias_of(h)
        for i in range(pairs):
            cols = lanes((side * heads + g) * pairs + i, span)
            out_ref[:, cols] = pair(qv[:, cols], bias)

    for g in range(heads):
        more = g + 1 < heads
        step(g, last)
        side_step(g, last)
        if g + 3 < heads:
            open_z(g + 3)
        if more:
            step(g + 1, 0)
        if g > 0:
            own_query(g - 1)
        if more:
            open_y(g + 1)
            side_step(g + 1, 0)
        take_far(g)
        if more:
            for t in range(1, last):
                step(g + 1, t)
                side_step(g + 1, t)
        close(g)
        far_query(g)
    own_query(heads - 1)

    for g in range(heads):
        drain(g)
    drain_rows()
    head_sent().wait_send()
    remote(qbuf, qbuf, qs, qr.at[0], (s, x_peer)).wait_send()
    results().wait_send()
    results().wait_recv()


def body(queries, keys, values, selected, counts, block_slot):
    ns = lax.axis_size("seq")
    nh = lax.axis_size("head")
    blk_seq, entries = selected.shape
    rows = queries.shape[0]
    heads = keys.shape[1] // HEAD_SIZE // 2
    width = queries.shape[1] // 2 // heads
    assert rows == BLOCK_ROWS and blk_seq == nh and nh == 4
    assert ns % Y_SIZE == 0 and ns > 2 * Y_SIZE and heads > 2
    hbm = pl.BlockSpec(memory_space=pl.ANY)
    zsz = ns // Y_SIZE
    dma = pltpu.SemaphoreType.DMA
    hops = max(zsz - 1, 1)
    held = zsz * (nh + PER_OWNER)
    big = [pltpu.with_memory_space_constraint(a, pltpu.HBM)
           for a in (queries, keys, values, selected, counts, block_slot)]
    return pl.pallas_call(
        functools.partial(kernel, ns, nh, heads, entries),
        out_shape=pltpu.VMEM(queries.shape, jnp.bfloat16),
        in_specs=[hbm] * 6,
        out_specs=pl.BlockSpec(memory_space=pltpu.VMEM),
        scratch_shapes=[
            pltpu.SMEM(selected.shape, jnp.int32),
            pltpu.SMEM(counts.shape, jnp.int32),
            pltpu.SMEM(block_slot.shape, jnp.int32),
            pltpu.VMEM(queries.shape, jnp.bfloat16),
            pltpu.VMEM((2,) + keys.shape, jnp.bfloat16),
            pltpu.VMEM((heads, rows, width), jnp.bfloat16),
            pltpu.VMEM((heads, rows, width), jnp.bfloat16),
            pltpu.VMEM((entries * BLOCK_ROWS, HEAD_SIZE), jnp.bfloat16),
            pltpu.VMEM((entries * BLOCK_ROWS, 2 * HEAD_SIZE), jnp.bfloat16),
            pltpu.VMEM((2 * BLOCK_ROWS, BLOCK_ROWS), jnp.float32),
            pltpu.VMEM((2, zsz * PER_OWNER, BLOCK_ROWS, HEAD_SIZE), jnp.bfloat16),
            pltpu.VMEM((Y_SIZE, zsz, 1, 128), jnp.int32),
            pltpu.SMEM((Y_SIZE, zsz, 1, 128), jnp.int32),
            pltpu.VMEM((8, 128), jnp.int32),
            pltpu.SMEM((8, 128), jnp.int32),
            pltpu.VMEM((8, 128), jnp.int32),
            pltpu.SMEM((8, 128), jnp.int32),
            dma((6,)), dma,
            dma, dma((heads, 2)),
            dma, dma((heads,)),
            dma((heads,)), dma((heads, 2, zsz)),
            dma((heads,)),
            dma((2,)), dma((heads,)),
            dma((heads,)), dma((heads,)),
            dma, dma,
            dma((1 + 2 * hops,)), dma((1 + 2 * hops,)),
        ] + [pltpu.VMEM((2, held, BLOCK_ROWS, HEAD_SIZE), jnp.bfloat16)] * heads,
        compiler_params=pltpu.CompilerParams(
            collective_id=0, has_side_effects=True, vmem_limit_bytes=60 * 1024 * 1024),
        name="block_attention",
    )(*big)


def solution(mesh):
    return jax.shard_map(
        body,
        mesh=mesh,
        in_specs=(
            P(("seq", "head"), None),
            P(("seq", "head"), None),
            P(("seq", "head"), None),
            P("seq", None),
            P("seq"),
            P("seq"),
        ),
        out_specs=P(("seq", "head"), None),
        check_vma=False,
    )
```
